32 devices in a mesh: depth: 8 (over y, x, core), rays: 4 (over z).
Axes of the slice: x: 2, y: 2, z: 4, core: 2. Of those that a mesh axis runs over, the one named last changes fastest.
Arguments:
- density: float32 [256, 65536], P('depth', 'rays'), may hold values from 0.0001953125 to 0.815625
- radiance: float32 [3, 256, 65536], P(None, 'depth', 'rays'), may hold values from 0 to 1
- target: float32 [3, 65536], P(None, 'rays'), may hold values from 0 to 1
Outputs:
- grad_density: float32 [256, 65536], P('depth', 'rays')
- loss_mean: float32 [], replicated
The draws below stay inside these ranges and needn't reach their ends.
All inputs are finite; a program needn't handle non-finite values.
Results may differ from the reference program's by a relative error of at most 0.0003.
Values sent between devices are 32-bit elements; how exact they have to be, the bound alone decides.
No kernel may reach another device: no remote copies, remote signals or barrier semaphores. Data moves between devices by JAX's collectives and lax.ppermute only.
A program may use at most 128 MiB of HBM per device.

```python
import math
import jax
import jax.numpy as jnp
from jax import lax

POINT_COUNT = 256
RAYS = 65536


def draw_density(key, part):
    base_key = jax.random.fold_in(key, 7301)
    first_key, second_key, third_key, fourth_key = jax.random.split(base_key, 4)
    starting_shift_amount = jnp.exp(jax.random.uniform(first_key, (POINT_COUNT, RAYS), jnp.float32, math.log(0.1), math.log(2.0)))
    multiplier_coefficient = jnp.exp(jax.random.uniform(second_key, (1, RAYS), jnp.float32, math.log(0.5), math.log(2.0)))
    location_numbers = jax.random.randint(third_key, (2, RAYS), 0, POINT_COUNT)
    elevation_levels = jax.random.uniform(fourth_key, (2, RAYS), jnp.float32, 0.15, 0.4)
    vertical_element = jnp.arange(POINT_COUNT, dtype=jnp.int32)[:, None]
    packet_clusters = jnp.where(vertical_element == location_numbers[0:1], elevation_levels[0:1], 0.0) + jnp.where(vertical_element == location_numbers[1:2], elevation_levels[1:2], 0.0)
    return (starting_shift_amount * multiplier_coefficient / POINT_COUNT + packet_clusters).astype(jnp.float32)


def shard_levels(stream_key, dims, pieces, smallest, high):
    def one(dim, blocks):
        draws = jax.random.uniform(jax.random.fold_in(jax.random.fold_in(stream_key, 6), dim), (blocks,), jnp.float32, smallest / len(pieces), high / len(pieces))
        return jnp.repeat(jnp.exp(draws), dims[dim] // blocks).reshape((-1,) + (1,) * (len(dims) - dim - 1))

    gain = one(*pieces[0])
    for cut in pieces[1:]:
        gain = gain * one(*cut)
    return gain


def setup_inputs(seed: int = 0) -> dict:
    keys = jax.random.split(jax.random.key(seed), 4)
    density = draw_density(jax.random.fold_in(keys[3], 71), 0)
    radiance = jnp.clip(1.0 * jax.random.uniform(keys[1], (3, POINT_COUNT, RAYS), jnp.float32) ** shard_levels(keys[1], (3, POINT_COUNT, RAYS), ((1, 8), (2, 4)), -0.2, 0.2), 0.0, 1.0)
    target = jnp.clip(1.0 * jax.random.uniform(keys[2], (3, RAYS), jnp.float32) ** shard_levels(keys[2], (3, RAYS), ((1, 4),), -0.2, 0.2), 0.0, 1.0)
    return dict(density=density, radiance=radiance, target=target)


def render_block(density, radiance, target):
    width = density.shape[1]
    zero_row = jnp.zeros((1, width), jnp.float32)
    zero_plane = jnp.zeros((3, 1, width), jnp.float32)
    sample_density = 0.5 * (density + jnp.concatenate([density[1:], zero_row], axis=0))
    sample_color = 0.5 * (radiance + jnp.concatenate([radiance[:, 1:], zero_plane], axis=1))
    running = jnp.cumsum(sample_density, axis=0)
    optical = jnp.concatenate([zero_row, running[:-1]], axis=0)
    transmit = jnp.exp(-optical)
    weight = transmit * (-jnp.expm1(-sample_density))
    emitted = weight[None] * sample_color
    prefix = jnp.cumsum(emitted, axis=1)
    pixel_color = prefix[:, -1]
    remaining = pixel_color[:, None, :] - prefix
    residual_grad = 2.0 * (pixel_color - target)
    transmit_next = transmit * jnp.exp(-sample_density)
    bracket = transmit_next[None] * sample_color - remaining
    sample_grad = jnp.sum(residual_grad[:, None, :] * bracket, axis=0)
    shifted = jnp.concatenate([zero_row, sample_grad[:-1]], axis=0)
    grad_block = 0.5 * (sample_grad + shifted)
    error_term = pixel_color - target
    return grad_block, jnp.sum(error_term * error_term)


def reference(density, radiance, target):
    block_rays = math.gcd(RAYS, 4096)
    block_count = RAYS // block_rays

    def render_one(block_index):
        start = (block_index * block_rays).astype(jnp.int32)
        part_density = lax.dynamic_slice_in_dim(density, start, block_rays, 1)
        part_radiance = lax.dynamic_slice_in_dim(radiance, start, block_rays, 2)
        part_target = lax.dynamic_slice_in_dim(target, start, block_rays, 1)
        return render_block(part_density, part_radiance, part_target)

    block_grads, losses = lax.map(render_one, jnp.arange(block_count, dtype=jnp.int32))
    grad_density = jnp.moveaxis(block_grads, 0, 1).reshape(POINT_COUNT, RAYS)
    loss_mean = jnp.sum(losses) / (3.0 * RAYS)
    return grad_density, loss_mean
```

```python
import jax
import jax.numpy as jnp
from jax import lax
from jax.experimental import pallas as pl
from jax.experimental.pallas import tpu as pltpu
from jax.sharding import PartitionSpec as P


SUB = 8
LANES = 128
BLOCKS = 16

OPACITY = (
    0.49999998698510023,
    -0.12499944339862339,
    0.020829460991082075,
    -0.0025942459011451765,
    0.00024876881447613667,
    -1.5181374461261048e-05,
)


def opacity_of(pair):
    value = OPACITY[-1]
    for factor in OPACITY[-2::-1]:
        value = value * pair + factor
    return value * pair


def edges_kernel(density, radiance, to_core, to_chip, sems):
    tiles = density.shape[0]

    def copies(row_in, row_out):
        first = [density.at[0, :, 0, :]] + [radiance.at[c, 0, :, 0, :] for c in range(3)]
        last = [density.at[tiles - 1, :, SUB - 1, :]]
        last += [radiance.at[c, tiles - 1, :, SUB - 1, :] for c in range(3)]
        made = []
        for at, source in enumerate(first):
            made.append(pltpu.make_async_copy(source, row_in.at[at], sems.at[at]))
        for at, source in enumerate(last):
            made.append(pltpu.make_async_copy(source, row_out.at[at], sems.at[4 + at]))
        return made

    even = lax.rem(lax.axis_index("depth"), 2) == 0

    @pl.when(even)
    def _():
        made = copies(to_chip, to_core)
        for copy in made:
            copy.start()
        for copy in made:
            copy.wait()

    @pl.when(jnp.logical_not(even))
    def _():
        made = copies(to_core, to_chip)
        for copy in made:
            copy.start()
        for copy in made:
            copy.wait()


def slab_kernel(density, radiance, out_h, out_state, out_last):
    tiles, blocks = density.shape[0], density.shape[1]
    samples = tiles * SUB
    rows = density.reshape(tiles * blocks * SUB, LANES)
    colors = radiance.reshape(3 * tiles * blocks * SUB, LANES)

    def cell(ref, plane, i):
        base = (plane * tiles + i // SUB) * blocks * SUB + i % SUB
        return ref[pl.ds(base, blocks, stride=SUB), :]

    here = cell(rows, 0, 0)
    color_here = [cell(colors, c, 0) for c in range(3)]
    transmit = None
    prefix = [None] * 3
    before = [None] * 3
    for i in range(samples - 1):
        after = cell(rows, 0, i + 1)
        opacity = opacity_of(here + after)
        here = after
        if i == 0:
            weight = opacity
            transmit = 1.0 - opacity
        else:
            weight = transmit * opacity
            transmit = transmit - weight
        for c in range(3):
            next_color = cell(colors, c, i + 1)
            color = color_here[c] + next_color
            color_here[c] = next_color
            seen = weight * color
            prefix[c] = seen if i == 0 else prefix[c] + seen
            value = transmit * color + prefix[c]
            out_h[0, c, i] = value if i == 0 else value + before[c]
            before[c] = value
    out_state[0] = transmit
    for c in range(3):
        out_state[1 + c] = prefix[c]
        out_last[c] = before[c]


def boundary_kernel(
    edge_core, edge_chip, rim_core, rim_chip, first, state, last, mine, other, h_first, h_last, full
):
    blocks = state.shape[1]
    half = blocks // 2
    parity = lax.rem(lax.axis_index("depth"), 2)
    even = parity == 0
    step = BLOCKS
    for at in range(0, blocks, step):
        part = pl.ds(at, step)
        density = jnp.where(even, edge_core[0, part], edge_chip[0, part])
        density = density + jnp.where(even, rim_core[0, part], rim_chip[0, part])
        opacity = opacity_of(density)
        transmit = state[0, part]
        weight = transmit * opacity
        transmit = transmit - weight
        full[0, part] = transmit
        for c in range(1, 4):
            own_last = jnp.where(even, edge_core[c, part], edge_chip[c, part])
            own_first = jnp.where(even, edge_chip[c, part], edge_core[c, part])
            behind = jnp.where(even, rim_core[c, part], rim_chip[c, part])
            ahead = jnp.where(even, rim_chip[c, part], rim_core[c, part])
            color = own_last + behind
            prefix = state[c, part] + weight * color
            full[c, part] = prefix
            h_last[c - 1, part] = last[c - 1, part] + transmit * color + prefix
            start = jnp.where(lax.axis_index("depth") == 0, 0.0, own_first + ahead)
            h_first[c - 1, part] = first[0, c - 1, 0, part] + start
    mine[...] = full[:, pl.ds(pl.multiple_of(parity * half, SUB), half), :]
    other[...] = full[:, pl.ds(pl.multiple_of((1 - parity) * half, SUB), half), :]


def grad_kernel(mine, other, h, h_first, h_last, out):
    tiles, blocks = out.shape[0], out.shape[1]
    samples = tiles * SUB
    half = mine.shape[1]
    at = pl.program_id(0) * blocks
    inside = pl.multiple_of(lax.rem(at, half), SUB)
    use_mine = at // half == lax.rem(lax.axis_index("depth"), 2)
    part = pl.ds(inside, blocks)
    a0, a1, a2, base = (jnp.where(use_mine, mine[c, part], other[c, part]) for c in range(4))
    base_first = jnp.where(lax.axis_index("depth") == 0, 0.5 * base, base)
    rows = out.reshape(tiles * blocks * SUB, LANES)
    for i in range(samples):
        if i == 0:
            h0, h1, h2 = h_first[0], h_first[1], h_first[2]
        elif i == samples - 1:
            h0, h1, h2 = h_last[0], h_last[1], h_last[2]
        else:
            h0, h1, h2 = h[0, 0, i], h[0, 1, i], h[0, 2, i]
        value = a0 * h0 + a1 * h1 + a2 * h2 - (base_first if i == 0 else base)
        rows[pl.ds((i // SUB) * blocks * SUB + i % SUB, blocks, stride=SUB), :] = value


def compose(front, back):
    return jnp.concatenate([front[:1] * back[:1], front[1:] + front[:1] * back[1:]], axis=0)


def stages(count):
    while count > 1:
        width = 4 if count % 4 == 0 else 2 if count % 2 == 0 else count
        yield width
        count //= width


def partner(device, stride, width, step):
    digit = device // stride % width
    source = digit ^ step if width & (width - 1) == 0 else (digit + step) % width
    return device + (source - digit) * stride


def on_device(density, radiance, target):
    samples, ray_count = density.shape
    devices = lax.axis_size("depth")
    index = lax.axis_index("depth")
    tiles, blocks = samples // SUB, ray_count // LANES
    half = blocks // 2
    even = index % 2 == 0
    f32 = jnp.float32

    def tiled(value):
        lead = value.shape[:-2]
        value = value.reshape(lead + (tiles, SUB, blocks, LANES))
        return jnp.swapaxes(value, -3, -2)

    density = tiled(density)
    radiance = tiled(radiance)
    swap = [(d, d ^ 1) for d in range(devices)]
    chain = [p for d in range(1, devices - 1, 2) for p in ((d, d + 1), (d + 1, d))]

    edge = jax.ShapeDtypeStruct((4, blocks, LANES), f32)
    whole = pl.BlockSpec(memory_space=pltpu.VMEM)
    anywhere = pl.BlockSpec(memory_space=pl.ANY)
    edge_core, edge_chip = pl.pallas_call(
        edges_kernel,
        out_shape=(edge, edge),
        in_specs=[anywhere, anywhere],
        out_specs=(whole, whole),
        scratch_shapes=[pltpu.SemaphoreType.DMA((8,))],
        name="edges",
    )(density, radiance)
    rim_chip = lax.ppermute(edge_chip, "depth", chain)
    rim_core = lax.ppermute(edge_core, "depth", swap)

    step = min(BLOCKS, half)
    grid = blocks // step
    kept = pltpu.CompilerParams(dimension_semantics=("arbitrary",))
    h, state, last = pl.pallas_call(
        slab_kernel,
        grid=(grid,),
        out_shape=(
            jax.ShapeDtypeStruct((grid, 3, samples - 1, step, LANES), f32),
            edge,
            jax.ShapeDtypeStruct((3, blocks, LANES), f32),
        ),
        in_specs=[
            pl.BlockSpec((tiles, step, SUB, LANES), lambda g: (0, g, 0, 0)),
            pl.BlockSpec((3, tiles, step, SUB, LANES), lambda g: (0, 0, g, 0, 0)),
        ],
        out_specs=(
            pl.BlockSpec((1, 3, samples - 1, step, LANES), lambda g: (g, 0, 0, 0, 0)),
            pl.BlockSpec((4, step, LANES), lambda g: (0, g, 0)),
            pl.BlockSpec((3, step, LANES), lambda g: (0, g, 0)),
        ),
        compiler_params=kept,
        cost_estimate=pl.CostEstimate(flops=40 * samples * ray_count, bytes_accessed=16 * samples * ray_count, transcendentals=0),
        name="slab",
    )(density, radiance)
    first = jnp.swapaxes(h[:, :, 0], 0, 1).reshape(1, 3, 1, blocks, LANES)

    part = jax.ShapeDtypeStruct((4, half, LANES), f32)
    row = jax.ShapeDtypeStruct((3, blocks, LANES), f32)
    mine, other, h_first, h_last = pl.pallas_call(
        boundary_kernel,
        out_shape=(part, part, row, row),
        in_specs=[whole] * 7,
        out_specs=(whole,) * 4,
        scratch_shapes=[pltpu.VMEM((4, blocks, LANES), f32)],
        name="boundary",
    )(edge_core, edge_chip, rim_core, rim_chip, first, state, last)

    theirs = lax.ppermute(other, "depth", swap)
    front = jnp.where(even, mine, theirs)
    back = jnp.where(even, theirs, mine)
    total = compose(front, back)
    before = None
    stride = 2
    for width in stages(devices // 2):
        members = [total] + [
            lax.ppermute(total, "depth", [(partner(d, stride, width, k), d) for d in range(devices)])
            for k in range(1, width)
        ]
        digit = index // stride % width
        ordered = []
        for place in range(width):
            picked = members[0]
            for k in range(1, width):
                source = digit ^ k if width & (width - 1) == 0 else (digit + k) % width
                picked = jnp.where(source == place, members[k], picked)
            ordered.append(picked)
        ahead = jnp.concatenate([jnp.ones_like(total[:1]), jnp.zeros_like(total[1:])], axis=0)
        running = ordered[0]
        for place in range(1, width):
            ahead = jnp.where(digit == place, running, ahead)
            running = compose(running, ordered[place])
        before = ahead if before is None else compose(ahead, before)
        total = running
        stride *= width

    parity = index % 2
    goal = target.reshape(3, 2, half, LANES)
    goal = jnp.where(even, goal[:, 0], goal[:, 1])
    error = 0.5 * total[1:] - goal
    loss = jnp.sum(error * error, axis=0)
    loss = jnp.sum(loss.reshape(half // SUB, SUB, LANES), axis=0)

    def scales(ahead):
        gain = 0.5 * ahead[:1] * error
        base = jnp.sum(error * (total[1:] - ahead[1:]), axis=0, keepdims=True)
        return jnp.concatenate([gain, base], axis=0)

    of_front = scales(before)
    of_back = scales(compose(before, front))
    scale_mine = jnp.where(even, of_front, of_back)
    scale_other = jnp.where(even, of_back, of_front)
    message = jnp.concatenate([scale_other.reshape(4 * half, LANES), loss], axis=0)
    received = lax.ppermute(message, "depth", swap)
    scale_theirs = received[: 4 * half].reshape(4, half, LANES)
    loss = loss + received[4 * half :]

    groups = lax.axis_size("rays")
    parts = [
        lax.ppermute(loss, "rays", [(d, (d + k) % groups) for d in range(groups)])
        for k in range(1, groups)
    ]

    grad = pl.pallas_call(
        grad_kernel,
        grid=(grid,),
        out_shape=jax.ShapeDtypeStruct((tiles, blocks, SUB, LANES), f32),
        in_specs=[
            pl.BlockSpec((4, half, LANES), lambda g: (0, 0, 0)),
            pl.BlockSpec((4, half, LANES), lambda g: (0, 0, 0)),
            pl.BlockSpec((1, 3, samples - 1, step, LANES), lambda g: (g, 0, 0, 0, 0)),
            pl.BlockSpec((3, step, LANES), lambda g: (0, g, 0)),
            pl.BlockSpec((3, step, LANES), lambda g: (0, g, 0)),
        ],
        out_specs=pl.BlockSpec((tiles, step, SUB, LANES), lambda g: (0, g, 0, 0)),
        compiler_params=kept,
        cost_estimate=pl.CostEstimate(flops=8 * samples * ray_count, bytes_accessed=16 * samples * ray_count, transcendentals=0),
        name="grad",
    )(scale_mine, scale_theirs, h, h_first, h_last)
    grad = jnp.swapaxes(grad, 1, 2).reshape(samples, ray_count)
    squares = loss
    for value in parts:
        squares = squares + value
    loss_mean = jnp.sum(squares) / (3.0 * ray_count * groups)
    return grad, loss_mean


def solution(mesh):
    in_specs = (P("depth", "rays"), P(None, "depth", "rays"), P(None, "rays"))
    out_specs = (P("depth", "rays"), P())
    return jax.shard_map(
        on_device, mesh=mesh, in_specs=in_specs, out_specs=out_specs, check_vma=False
    )
```

```python
import functools

import jax
import jax.numpy as jnp
from jax import lax
from jax.experimental import pallas as pl
from jax.experimental.pallas import tpu as pltpu
from jax.sharding import PartitionSpec as P


SUB = 8
LANES = 128
BLOCKS = 16
EDGES = 52 << 20
KEPT = 20 << 20
SMALL = 8 << 20

OPACITY = (
    0.49999998698510023,
    -0.12499944339862339,
    0.020829460991082075,
    -0.0025942459011451765,
    0.00024876881447613667,
    -1.5181374461261048e-05,
)


def opacity_of(pair):
    value = OPACITY[-1]
    for factor in OPACITY[-2::-1]:
        value = value * pair + factor
    return value * pair


def edges_kernel(density, radiance, to_core, to_chip, sems):
    tiles = density.shape[0]

    def copies(row_in, row_out):
        first = [density.at[0, :, 0, :]] + [radiance.at[c, 0, :, 0, :] for c in range(3)]
        last = [density.at[tiles - 1, :, SUB - 1, :]]
        last += [radiance.at[c, tiles - 1, :, SUB - 1, :] for c in range(3)]
        made = []
        for at, source in enumerate(first):
            made.append(pltpu.make_async_copy(source, row_in.at[at], sems.at[at]))
        for at, source in enumerate(last):
            made.append(pltpu.make_async_copy(source, row_out.at[at], sems.at[4 + at]))
        return made

    even = lax.rem(lax.axis_index("depth"), 2) == 0

    @pl.when(even)
    def _():
        made = copies(to_chip, to_core)
        for copy in made:
            copy.start()
        for copy in made:
            copy.wait()

    @pl.when(jnp.logical_not(even))
    def _():
        made = copies(to_core, to_chip)
        for copy in made:
            copy.start()
        for copy in made:
            copy.wait()


def slab_kernel(density, radiance, out_h, out_state, out_first, out_last):
    tiles, blocks = density.shape[0], density.shape[1]
    samples = tiles * SUB
    step = BLOCKS
    rows = density.reshape(tiles * blocks * SUB, LANES)
    planes = radiance.reshape(3 * tiles * blocks * SUB, LANES)

    @pl.loop(0, blocks // step)
    def _(g):
        part = pl.ds(pl.multiple_of(g * step, step), step)

        def cell(ref, plane, i):
            base = (plane * tiles + i // SUB) * blocks * SUB + i % SUB
            base = pl.multiple_of(g * (step * SUB), SUB) + base
            return ref[pl.ds(base, step, stride=SUB), :]

        here = cell(rows, 0, 0)
        color_here = [cell(planes, c, 0) for c in range(3)]
        transmit = None
        prefix = [None] * 3
        before = [None] * 3
        for i in range(samples - 1):
            after = cell(rows, 0, i + 1)
            opacity = opacity_of(here + after)
            here = after
            if i == 0:
                weight = opacity
                transmit = 1.0 - opacity
            else:
                weight = transmit * opacity
                transmit = transmit - weight
            for c in range(3):
                next_color = cell(planes, c, i + 1)
                color = color_here[c] + next_color
                color_here[c] = next_color
                seen = weight * color
                prefix[c] = seen if i == 0 else prefix[c] + seen
                value = transmit * color + prefix[c]
                if i == 0:
                    out_first[c, part] = value
                else:
                    out_h[g, c, i - 1] = value + before[c]
                before[c] = value
        out_state[0, part] = transmit
        for c in range(3):
            out_state[1 + c, part] = prefix[c]
            out_last[c, part] = before[c]


def boundary_kernel(
    edge_core, edge_chip, rim_core, rim_chip, first, state, last, mine, other, h_first, h_last, full
):
    blocks = state.shape[1]
    half = blocks // 2
    parity = lax.rem(lax.axis_index("depth"), 2)
    even = parity == 0
    step = BLOCKS
    for at in range(0, blocks, step):
        part = pl.ds(at, step)
        density = jnp.where(even, edge_core[0, part], edge_chip[0, part])
        density = density + jnp.where(even, rim_core[0, part], rim_chip[0, part])
        opacity = opacity_of(density)
        transmit = state[0, part]
        weight = transmit * opacity
        transmit = transmit - weight
        full[0, part] = transmit
        for c in range(1, 4):
            own_last = jnp.where(even, edge_core[c, part], edge_chip[c, part])
            own_first = jnp.where(even, edge_chip[c, part], edge_core[c, part])
            behind = jnp.where(even, rim_core[c, part], rim_chip[c, part])
            ahead = jnp.where(even, rim_chip[c, part], rim_core[c, part])
            color = own_last + behind
            prefix = state[c, part] + weight * color
            full[c, part] = prefix
            h_last[c - 1, part] = last[c - 1, part] + transmit * color + prefix
            start = jnp.where(lax.axis_index("depth") == 0, 0.0, own_first + ahead)
            h_first[c - 1, part] = first[c - 1, part] + start
    mine[...] = full[:, pl.ds(pl.multiple_of(parity * half, SUB), half), :]
    other[...] = full[:, pl.ds(pl.multiple_of((1 - parity) * half, SUB), half), :]


def grad_kernel(mine, other, h, h_first, h_last, out):
    tiles, blocks = out.shape[0], out.shape[1]
    samples = tiles * SUB
    half = mine.shape[1]
    at = pl.program_id(0) * blocks
    inside = pl.multiple_of(lax.rem(at, half), SUB)
    use_mine = at // half == lax.rem(lax.axis_index("depth"), 2)
    part = pl.ds(inside, blocks)
    outer = pl.ds(pl.multiple_of(at, SUB), blocks)
    a0, a1, a2, base = (jnp.where(use_mine, mine[c, part], other[pl.ds(c * half + inside, blocks), :]) for c in range(4))
    base_first = jnp.where(lax.axis_index("depth") == 0, 0.5 * base, base)
    rows = out.reshape(tiles * blocks * SUB, LANES)
    for i in range(samples):
        if i == 0:
            h0, h1, h2 = (h_first[c, outer] for c in range(3))
        elif i == samples - 1:
            h0, h1, h2 = (h_last[c, outer] for c in range(3))
        else:
            h0, h1, h2 = (h[pl.program_id(0), c, i - 1] for c in range(3))
        value = a0 * h0 + a1 * h1 + a2 * h2 - (base_first if i == 0 else base)
        rows[pl.ds((i // SUB) * blocks * SUB + i % SUB, blocks, stride=SUB), :] = value


def compose(front, back):
    return [front[0] * back[0]] + [front[c] + front[0] * back[c] for c in range(1, 4)]


def chosen(flag, yes, no):
    return [jnp.where(flag, a, b) for a, b in zip(yes, no, strict=True)]


def chip_kernel(mine, theirs, out):
    even = lax.rem(lax.axis_index("depth"), 2) == 0
    for at in range(0, out.shape[1], BLOCKS):
        part = pl.ds(at, BLOCKS)
        own = [mine[c, part] for c in range(4)]
        far = [theirs[c, part] for c in range(4)]
        total = compose(chosen(even, own, far), chosen(even, far, own))
        for c in range(4):
            out[c, part] = total[c]


def gathered(members, earlier, part, stride):
    width = len(members)
    digit = lax.rem(lax.div(lax.axis_index("depth"), stride), width)
    values = [[member[c, part] for c in range(4)] for member in members]
    ordered = []
    for place in range(width):
        picked = values[0]
        for k in range(1, width):
            source = digit ^ k if width & (width - 1) == 0 else lax.rem(digit + k, width)
            picked = chosen(source == place, values[k], picked)
        ordered.append(picked)
    one = jnp.ones_like(values[0][0])
    ahead = [one] + [jnp.zeros_like(one)] * 3
    total = ordered[0]
    for place in range(1, width):
        ahead = chosen(digit == place, total, ahead)
        total = compose(total, ordered[place])
    if earlier is not None:
        ahead = compose(ahead, [earlier[c, part] for c in range(4)])
    return ahead, total


def stage_kernel(stride, width, started, *refs):
    members = refs[:width]
    earlier = refs[width] if started else None
    out_ahead, out_total = refs[-2:]
    for at in range(0, out_total.shape[1], BLOCKS):
        part = pl.ds(at, BLOCKS)
        ahead, total = gathered(members, earlier, part, stride)
        for c in range(4):
            out_ahead[c, part] = ahead[c]
            out_total[c, part] = total[c]


def scale_kernel(stride, width, started, mine, theirs, target, *refs):
    members = refs[:width]
    earlier = refs[width] if started else None
    out_mine, out_message, out_loss = refs[-3:]
    half = out_mine.shape[1]
    parity = lax.rem(lax.axis_index("depth"), 2)
    even = parity == 0
    loss = None
    for at in range(0, half, BLOCKS):
        part = pl.ds(at, BLOCKS)
        before, total = gathered(members, earlier, part, stride)
        own = [mine[c, part] for c in range(4)]
        far = [theirs[c, part] for c in range(4)]
        behind = compose(before, chosen(even, own, far))
        goal = pl.ds(pl.multiple_of(parity * half + at, SUB), BLOCKS)
        error = [0.5 * total[c] - target[c - 1, goal] for c in range(1, 4)]
        squares = error[0] * error[0] + error[1] * error[1] + error[2] * error[2]
        loss = squares if loss is None else loss + squares
        for ahead, is_own in ((before, even), (behind, jnp.logical_not(even))):
            gain = 0.5 * ahead[0]
            values = [gain * error[c] for c in range(3)]
            base = error[0] * (total[1] - ahead[1])
            for c in (1, 2):
                base = base + error[c] * (total[1 + c] - ahead[1 + c])
            values.append(base)

            @pl.when(is_own)
            def _():
                for c in range(4):
                    out_mine[c, part] = values[c]

            @pl.when(jnp.logical_not(is_own))
            def _():
                for c in range(4):
                    out_message[pl.ds(c * half + at, BLOCKS), :] = values[c]

    folded = sum(loss[at : at + SUB] for at in range(0, BLOCKS, SUB))
    folded = jnp.full((SUB, LANES), jnp.sum(folded), jnp.float32)
    out_message[pl.ds(4 * half, SUB), :] = folded
    out_loss[...] = folded


def stages(count):
    while count > 1:
        width = 4 if count % 4 == 0 else 2 if count % 2 == 0 else count
        yield width
        count //= width


def partner(device, stride, width, step):
    digit = device // stride % width
    source = digit ^ step if width & (width - 1) == 0 else (digit + step) % width
    return device + (source - digit) * stride


def on_device(density, radiance, target):
    samples, ray_count = density.shape
    devices = lax.axis_size("depth")
    tiles, blocks = samples // SUB, ray_count // LANES
    half = blocks // 2
    f32 = jnp.float32

    def tiled(value):
        lead = value.shape[:-2]
        value = value.reshape(lead + (tiles, SUB, blocks, LANES))
        return jnp.swapaxes(value, -3, -2)

    density = tiled(density)
    radiance = tiled(radiance)
    swap = [(d, d ^ 1) for d in range(devices)]
    chain = [p for d in range(1, devices - 1, 2) for p in ((d, d + 1), (d + 1, d))]

    edge = jax.ShapeDtypeStruct((4, blocks, LANES), f32)
    row = jax.ShapeDtypeStruct((3, blocks, LANES), f32)
    whole = pl.BlockSpec(memory_space=pltpu.VMEM)
    stays = pl.BlockSpec(memory_space=pltpu.HBM)
    edge_core, edge_chip = pl.pallas_call(
        edges_kernel,
        out_shape=(edge, edge),
        in_specs=[stays, stays],
        out_specs=(whole, whole),
        scratch_shapes=[pltpu.SemaphoreType.DMA((8,))],
        compiler_params=pltpu.CompilerParams(vmem_limit_bytes=EDGES),
        name="edges",
    )(density, radiance)
    rim_chip = lax.ppermute(edge_chip, "depth", chain)
    rim_core = lax.ppermute(edge_core, "depth", swap)

    step = BLOCKS
    grid = blocks // step
    h, state, first, last = pl.pallas_call(
        slab_kernel,
        out_shape=(
            jax.ShapeDtypeStruct((grid, 3, samples - 2, step, LANES), f32),
            edge,
            row,
            row,
        ),
        in_specs=[whole, whole],
        out_specs=(whole,) * 4,
        compiler_params=pltpu.CompilerParams(vmem_limit_bytes=KEPT),
        cost_estimate=pl.CostEstimate(
            flops=40 * samples * ray_count,
            bytes_accessed=16 * samples * ray_count,
            transcendentals=0,
        ),
        name="slab",
    )(density, radiance)

    part = jax.ShapeDtypeStruct((4, half, LANES), f32)
    mine, other, h_first, h_last = pl.pallas_call(
        boundary_kernel,
        out_shape=(part, part, row, row),
        in_specs=[whole] * 7,
        out_specs=(whole,) * 4,
        scratch_shapes=[pltpu.VMEM((4, blocks, LANES), f32)],
        compiler_params=pltpu.CompilerParams(vmem_limit_bytes=KEPT),
        name="boundary",
    )(edge_core, edge_chip, rim_core, rim_chip, first, state, last)

    small = pltpu.CompilerParams(vmem_limit_bytes=SMALL)
    theirs = lax.ppermute(other, "depth", swap)
    total = pl.pallas_call(
        chip_kernel,
        out_shape=part,
        in_specs=[whole, whole],
        out_specs=whole,
        compiler_params=small,
        name="chip",
    )(mine, theirs)
    goal = target.reshape(3, blocks, LANES)
    earlier = ()
    stride = 2
    widths = list(stages(devices // 2)) or [1]
    for at, width in enumerate(widths):
        members = [total] + [
            lax.ppermute(total, "depth", [(partner(d, stride, width, k), d) for d in range(devices)])
            for k in range(1, width)
        ]
        last_stage = at == len(widths) - 1
        if last_stage:
            body = functools.partial(scale_kernel, stride, width, bool(earlier))
            given = (mine, theirs, goal, *members, *earlier)
            made = (
                part,
                jax.ShapeDtypeStruct((4 * half + SUB, LANES), f32),
                jax.ShapeDtypeStruct((SUB, LANES), f32),
            )
        else:
            body = functools.partial(stage_kernel, stride, width, bool(earlier))
            given = (*members, *earlier)
            made = (part, part)
        results = pl.pallas_call(
            body,
            out_shape=made,
            in_specs=[whole] * len(given),
            out_specs=(whole,) * len(made),
            compiler_params=small,
            name="scale" if last_stage else "stage",
        )(*given)
        if not last_stage:
            earlier, total = (results[0],), results[1]
        stride *= width
    scale_mine, message, loss = results

    received = lax.ppermute(message, "depth", swap)
    loss = loss + received[4 * half :]

    groups = lax.axis_size("rays")
    parts = [
        lax.ppermute(loss, "rays", [(d, (d + k) % groups) for d in range(groups)])
        for k in range(1, groups)
    ]

    grad = pl.pallas_call(
        grad_kernel,
        grid=(grid,),
        out_shape=jax.ShapeDtypeStruct((tiles, blocks, SUB, LANES), f32),
        in_specs=[
            whole,
            whole,
            whole,
            whole,
            whole,
        ],
        out_specs=pl.BlockSpec((tiles, step, SUB, LANES), lambda g: (0, g, 0, 0)),
        compiler_params=pltpu.CompilerParams(vmem_limit_bytes=KEPT),
        cost_estimate=pl.CostEstimate(
            flops=8 * samples * ray_count,
            bytes_accessed=16 * samples * ray_count,
            transcendentals=0,
        ),
        name="grad",
    )(scale_mine, received, h, h_first, h_last)
    grad = jnp.swapaxes(grad, 1, 2).reshape(samples, ray_count)
    squares = loss
    for value in parts:
        squares = squares + value
    loss_mean = squares[0, 0] / (3.0 * ray_count * groups)
    return grad, loss_mean


def solution(mesh):
    in_specs = (P("depth", "rays"), P(None, "depth", "rays"), P(None, "rays"))
    out_specs = (P("depth", "rays"), P())
    return jax.shard_map(
        on_device, mesh=mesh, in_specs=in_specs, out_specs=out_specs, check_vma=False
    )
```

```python
import functools

import jax
import jax.numpy as jnp
from jax import lax
from jax.experimental import pallas as pl
from jax.experimental.pallas import tpu as pltpu
from jax.sharding import PartitionSpec as P


SUB = 8
LANES = 128
BLOCKS = 16
EDGES = 52 << 20
KEPT = 20 << 20
SMALL = 8 << 20

OPACITY = (
    0.49999998698510023,
    -0.12499944339862339,
    0.020829460991082075,
    -0.0025942459011451765,
    0.00024876881447613667,
    -1.5181374461261048e-05,
)


def opacity_of(pair):
    value = OPACITY[-1]
    for factor in OPACITY[-2::-1]:
        value = value * pair + factor
    return value * pair


def edge_kernel(density, radiance, out, sems):
    rows = [density.at[0, :, 0, :]] + [radiance.at[c, 0, :, 0, :] for c in range(3)]
    copies = [pltpu.make_async_copy(row, out.at[at], sems.at[at]) for at, row in enumerate(rows)]
    for copy in copies:
        copy.start()
    for copy in copies:
        copy.wait()


def slab_kernel(density, radiance, out_h, out_state, out_first, out_last, out_cell, out_colors):
    tiles, blocks = density.shape[0], density.shape[1]
    samples = tiles * SUB
    step = BLOCKS
    rows = density.reshape(tiles * blocks * SUB, LANES)
    planes = radiance.reshape(3 * tiles * blocks * SUB, LANES)

    @pl.loop(0, blocks // step)
    def _(g):
        part = pl.ds(pl.multiple_of(g * step, step), step)

        def cell(ref, plane, i):
            base = (plane * tiles + i // SUB) * blocks * SUB + i % SUB
            base = pl.multiple_of(g * (step * SUB), SUB) + base
            return ref[pl.ds(base, step, stride=SUB), :]

        here = cell(rows, 0, 0)
        color_here = [cell(planes, c, 0) for c in range(3)]
        transmit = None
        prefix = [None] * 3
        before = [None] * 3
        for i in range(samples - 1):
            after = cell(rows, 0, i + 1)
            opacity = opacity_of(here + after)
            here = after
            if i == 0:
                weight = opacity
                transmit = 1.0 - opacity
            else:
                weight = transmit * opacity
                transmit = transmit - weight
            for c in range(3):
                next_color = cell(planes, c, i + 1)
                color = color_here[c] + next_color
                color_here[c] = next_color
                seen = weight * color
                prefix[c] = seen if i == 0 else prefix[c] + seen
                value = transmit * color + prefix[c]
                if i == 0:
                    out_first[c, part] = value
                else:
                    out_h[g, c, i - 1] = value + before[c]
                before[c] = value
        out_cell[0, part] = here
        out_state[0, part] = transmit
        for c in range(3):
            out_state[1 + c, part] = prefix[c]
            out_last[c, part] = before[c]
            out_colors[c, part] = color_here[c]


def boundary_kernel(cell, colors, behind, state, last, mine, other, h_last, full):
    blocks = state.shape[1]
    half = blocks // 2
    parity = lax.rem(lax.axis_index("depth"), 2)
    for at in range(0, blocks, BLOCKS):
        part = pl.ds(at, BLOCKS)
        opacity = opacity_of(cell[0, part] + behind[0, part])
        transmit = state[0, part]
        weight = transmit * opacity
        transmit = transmit - weight
        full[0, part] = transmit
        for c in range(3):
            color = colors[c, part] + behind[1 + c, part]
            prefix = state[1 + c, part] + weight * color
            full[1 + c, part] = prefix
            h_last[c, part] = last[c, part] + transmit * color + prefix
    mine[...] = full[:, pl.ds(pl.multiple_of(parity * half, SUB), half), :]
    other[...] = full[:, pl.ds(pl.multiple_of((1 - parity) * half, SUB), half), :]


def grad_kernel(own, scales, h, first, edge, ahead, h_last, *refs):
    out, buffers, sems = refs[-3:]
    tiles, blocks = out.shape[0], out.shape[1]
    samples = tiles * SUB
    half = blocks // 2
    step = BLOCKS
    index = lax.axis_index("depth")
    parity = lax.rem(index, 2)
    start = pl.multiple_of((parity if own else 1 - parity) * half, step)
    count = half // step

    def copy(k):
        part = pl.ds(pl.multiple_of(start + k * step, step), step)
        return pltpu.make_async_copy(buffers.at[k], out.at[:, part], sems.at[k])

    @pl.loop(0, count)
    def _(k):
        inside = pl.ds(pl.multiple_of(k * step, step), step)
        part = pl.ds(pl.multiple_of(start + k * step, step), step)
        group = lax.div(start, step) + k
        a0, a1, a2, base = (scales[c, inside] for c in range(4))
        rows = buffers.at[k].reshape(tiles * step * SUB, LANES)
        for i in range(samples):
            away = base
            if i == 0:
                h0, h1, h2 = (
                    first[c, part]
                    + jnp.where(index == 0, 0.0, edge[1 + c, part] + ahead[c, part])
                    for c in range(3)
                )
                away = jnp.where(index == 0, 0.5 * base, base)
            elif i == samples - 1:
                h0, h1, h2 = (h_last[c, part] for c in range(3))
            else:
                h0, h1, h2 = (h[group, c, i - 1] for c in range(3))
            value = a0 * h0 + a1 * h1 + a2 * h2 - away
            rows[pl.ds((i // SUB) * step * SUB + i % SUB, step, stride=SUB), :] = value
        copy(k).start()

    @pl.loop(0, count)
    def _(k):
        copy(k).wait()


def sent(value, axis, pairs):
    return lax.ppermute(value, axis, pairs)


def compose(front, back):
    return [front[0] * back[0]] + [front[c] + front[0] * back[c] for c in range(1, 4)]


def chosen(flag, yes, no):
    return [jnp.where(flag, a, b) for a, b in zip(yes, no, strict=True)]


def chip_kernel(mine, theirs, out):
    even = lax.rem(lax.axis_index("depth"), 2) == 0
    for at in range(0, out.shape[1], BLOCKS):
        part = pl.ds(at, BLOCKS)
        own = [mine[c, part] for c in range(4)]
        far = [theirs[c, part] for c in range(4)]
        total = compose(chosen(even, own, far), chosen(even, far, own))
        for c in range(4):
            out[c, part] = total[c]


def gathered(members, earlier, part, stride):
    width = len(members)
    digit = lax.rem(lax.div(lax.axis_index("depth"), stride), width)
    values = [[member[c, part] for c in range(4)] for member in members]
    ordered = []
    for place in range(width):
        picked = values[0]
        for k in range(1, width):
            source = digit ^ k if width & (width - 1) == 0 else lax.rem(digit + k, width)
            picked = chosen(source == place, values[k], picked)
        ordered.append(picked)
    one = jnp.ones_like(values[0][0])
    ahead = [one] + [jnp.zeros_like(one)] * 3
    total = ordered[0]
    for place in range(1, width):
        ahead = chosen(digit == place, total, ahead)
        total = compose(total, ordered[place])
    if earlier is not None:
        ahead = compose(ahead, [earlier[c, part] for c in range(4)])
    return ahead, total


def stage_kernel(stride, width, started, *refs):
    members = refs[:width]
    earlier = refs[width] if started else None
    out_ahead, out_total = refs[-2:]
    for at in range(0, out_total.shape[1], BLOCKS):
        part = pl.ds(at, BLOCKS)
        ahead, total = gathered(members, earlier, part, stride)
        for c in range(4):
            out_ahead[c, part] = ahead[c]
            out_total[c, part] = total[c]


def scale_kernel(stride, width, started, mine, theirs, target, *refs):
    members = refs[:width]
    earlier = refs[width] if started else None
    out_mine, out_other, out_loss = refs[-3:]
    half = out_mine.shape[1]
    parity = lax.rem(lax.axis_index("depth"), 2)
    even = parity == 0
    loss = None
    for at in range(0, half, BLOCKS):
        part = pl.ds(at, BLOCKS)
        before, total = gathered(members, earlier, part, stride)
        own = [mine[c, part] for c in range(4)]
        far = [theirs[c, part] for c in range(4)]
        behind = compose(before, chosen(even, own, far))
        goal = pl.ds(pl.multiple_of(parity * half + at, SUB), BLOCKS)
        error = [0.5 * total[c] - target[c - 1, goal] for c in range(1, 4)]
        squares = error[0] * error[0] + error[1] * error[1] + error[2] * error[2]
        loss = squares if loss is None else loss + squares
        for ahead, is_own in ((before, even), (behind, jnp.logical_not(even))):
            gain = 0.5 * ahead[0]
            values = [gain * error[c] for c in range(3)]
            base = error[0] * (total[1] - ahead[1])
            for c in (1, 2):
                base = base + error[c] * (total[1 + c] - ahead[1 + c])
            values.append(base)

            @pl.when(is_own)
            def _():
                for c in range(4):
                    out_mine[c, part] = values[c]

            @pl.when(jnp.logical_not(is_own))
            def _():
                for c in range(4):
                    out_other[c, part] = values[c]

    out_loss[...] = jnp.full(out_loss.shape, jnp.sum(loss), jnp.float32)


def stages(count):
    while count > 1:
        width = 4 if count % 4 == 0 else 2 if count % 2 == 0 else count
        yield width
        count //= width


def ring_sum(count):
    if count == 4:
        return [[[(0, 1), (1, 0), (2, 3), (3, 2)]], [[(1, 2), (2, 1), (3, 0), (0, 3)]]]
    if count & (count - 1) == 0 and count > 1:
        steps = [1 << bit for bit in range(count.bit_length() - 1)]
        return [[[(d, d ^ step) for d in range(count)]] for step in steps]
    return [[[(d, (d + k) % count) for d in range(count)] for k in range(1, count)]]


def partner(device, stride, width, step):
    digit = device // stride % width
    source = digit ^ step if width & (width - 1) == 0 else (digit + step) % width
    return device + (source - digit) * stride


def on_device(density, radiance, target):
    samples, ray_count = density.shape
    devices = lax.axis_size("depth")
    tiles, blocks = samples // SUB, ray_count // LANES
    half = blocks // 2
    f32 = jnp.float32

    def tiled(value):
        lead = value.shape[:-2]
        value = value.reshape(lead + (tiles, SUB, blocks, LANES))
        return jnp.swapaxes(value, -3, -2)

    density = tiled(density)
    radiance = tiled(radiance)
    swap = [(d, d ^ 1) for d in range(devices)]

    row = jax.ShapeDtypeStruct((1, blocks, LANES), f32)
    colors = jax.ShapeDtypeStruct((3, blocks, LANES), f32)
    edge = jax.ShapeDtypeStruct((4, blocks, LANES), f32)
    whole = pl.BlockSpec(memory_space=pltpu.VMEM)
    stays = pl.BlockSpec(memory_space=pl.ANY)
    first_row = pl.pallas_call(
        edge_kernel,
        out_shape=edge,
        in_specs=[stays, stays],
        out_specs=whole,
        scratch_shapes=[pltpu.SemaphoreType.DMA((4,))],
        compiler_params=pltpu.CompilerParams(vmem_limit_bytes=EDGES),
        name="edge",
    )(density, radiance)
    behind = sent(first_row, "depth", [(d + 1, d) for d in range(devices - 1)])

    step = BLOCKS
    grid = blocks // step
    h, state, first, last, last_cell, last_colors = pl.pallas_call(
        slab_kernel,
        out_shape=(
            jax.ShapeDtypeStruct((grid, 3, samples - 2, step, LANES), f32),
            edge,
            colors,
            colors,
            row,
            colors,
        ),
        in_specs=[whole, whole],
        out_specs=(whole,) * 6,
        compiler_params=pltpu.CompilerParams(vmem_limit_bytes=KEPT),
        cost_estimate=pl.CostEstimate(
            flops=40 * samples * ray_count,
            bytes_accessed=16 * samples * ray_count,
            transcendentals=0,
        ),
        name="slab",
    )(density, radiance)

    part = jax.ShapeDtypeStruct((4, half, LANES), f32)
    ahead = sent(last_colors, "depth", [(d, d + 1) for d in range(devices - 1)])
    mine, other, h_last = pl.pallas_call(
        boundary_kernel,
        out_shape=(part, part, colors),
        in_specs=[whole] * 5,
        out_specs=(whole,) * 3,
        scratch_shapes=[pltpu.VMEM((4, blocks, LANES), f32)],
        compiler_params=pltpu.CompilerParams(vmem_limit_bytes=KEPT),
        name="boundary",
    )(last_cell, last_colors, behind, state, last)

    small = pltpu.CompilerParams(vmem_limit_bytes=SMALL)
    theirs = sent(other, "depth", swap)
    total = pl.pallas_call(
        chip_kernel,
        out_shape=part,
        in_specs=[whole, whole],
        out_specs=whole,
        compiler_params=small,
        name="chip",
    )(mine, theirs)
    goal = target.reshape(3, blocks, LANES)
    earlier = ()
    stride = 2
    widths = list(stages(devices // 2)) or [1]
    for at, width in enumerate(widths):
        members = [total] + [
            sent(total, "depth", [(partner(d, stride, width, k), d) for d in range(devices)])
            for k in range(1, width)
        ]
        last_stage = at == len(widths) - 1
        if last_stage:
            body = functools.partial(scale_kernel, stride, width, bool(earlier))
            given = (mine, theirs, goal, *members, *earlier)
            made = (
                part,
                part,
                jax.ShapeDtypeStruct((SUB, LANES), f32),
            )
        else:
            body = functools.partial(stage_kernel, stride, width, bool(earlier))
            given = (*members, *earlier)
            made = (part, part)
        results = pl.pallas_call(
            body,
            out_shape=made,
            in_specs=[whole] * len(given),
            out_specs=(whole,) * len(made),
            compiler_params=small,
            name="scale" if last_stage else "stage",
        )(*given)
        if not last_stage:
            earlier, total = (results[0],), results[1]
        stride *= width
    scale_mine, scale_other, loss = results

    def grad_half(own, scales, *before):
        return pl.pallas_call(
            functools.partial(grad_kernel, own),
            out_shape=jax.ShapeDtypeStruct((tiles, blocks, SUB, LANES), f32),
            in_specs=[whole] * 6 + [stays] * len(before),
            out_specs=stays,
            input_output_aliases={6: 0} if before else {},
            scratch_shapes=[
                pltpu.VMEM((grid // 2, tiles, step, SUB, LANES), f32),
                pltpu.SemaphoreType.DMA((grid // 2,)),
            ],
            compiler_params=pltpu.CompilerParams(vmem_limit_bytes=KEPT),
            cost_estimate=pl.CostEstimate(
                flops=4 * samples * ray_count,
                bytes_accessed=8 * samples * ray_count,
                transcendentals=0,
            ),
            name="grad",
        )(scales, h, first, first_row, ahead, h_last, *before)

    scale_theirs = sent(scale_other, "depth", swap)
    groups = lax.axis_size("rays")
    rounds = ring_sum(groups)
    for at, pairs in enumerate(rounds):
        others = [sent(loss, "rays", pair) for pair in pairs]
        if at == 0:
            grad = grad_half(True, scale_mine)
        loss = sum(others, loss)
        if at == 0:
            loss = loss + sent(loss, "depth", swap)
            grad = grad_half(False, scale_theirs, grad)
    grad = jnp.swapaxes(grad, 1, 2).reshape(samples, ray_count)
    return grad, loss[0, 0] / (3.0 * ray_count * groups)


def solution(mesh):
    in_specs = (P("depth", "rays"), P(None, "depth", "rays"), P(None, "rays"))
    out_specs = (P("depth", "rays"), P())
    return jax.shard_map(
        on_device, mesh=mesh, in_specs=in_specs, out_specs=out_specs, check_vma=False
    )
```

```python
import functools
import math

import jax
import jax.numpy as jnp
from jax import lax
from jax.experimental import pallas as pl
from jax.experimental.pallas import tpu as pltpu
from jax.sharding import PartitionSpec as P


SUB = 8
LANES = 128
BLOCKS = 16
EDGES = 52 << 20
KEPT = 20 << 20
SMALL = 8 << 20

OPACITY = (
    0.49999998698510023,
    -0.12499944339862339,
    0.020829460991082075,
    -0.0025942459011451765,
    0.00024876881447613667,
    -1.5181374461261048e-05,
)


def opacity_of(pair):
    value = OPACITY[-1]
    for factor in OPACITY[-2::-1]:
        value = value * pair + factor
    return value * pair


def is_even():
    return lax.rem(lax.axis_index("depth"), 2) == 0


def edge_kernel(density, unused, to_core, to_chip, rows, sems):
    tiles = density.shape[0]
    first = pltpu.make_async_copy(density.at[0, :, 0, :], rows.at[0], sems.at[0])
    last = pltpu.make_async_copy(density.at[tiles - 1, :, SUB - 1, :], rows.at[1], sems.at[1])
    first.start()
    last.start()
    first.wait()
    last.wait()
    even = is_even()
    to_core[0] = jnp.where(even, rows[1], rows[0])
    to_chip[0] = jnp.where(even, rows[0], rows[1])


def slab_kernel(density, radiance, out_h, out_state, out_first, out_last, to_core, to_chip):
    tiles, blocks = density.shape[0], density.shape[1]
    samples = tiles * SUB
    step = BLOCKS
    rows = density.reshape(tiles * blocks * SUB, LANES)
    planes = radiance.reshape(3 * tiles * blocks * SUB, LANES)

    @pl.loop(0, blocks // step)
    def _(g):
        part = pl.ds(pl.multiple_of(g * step, step), step)

        def cell(ref, plane, i):
            base = (plane * tiles + i // SUB) * blocks * SUB + i % SUB
            base = pl.multiple_of(g * (step * SUB), SUB) + base
            return ref[pl.ds(base, step, stride=SUB), :]

        here = cell(rows, 0, 0)
        color_here = [cell(planes, c, 0) for c in range(3)]
        even = is_even()
        color_first = list(color_here)
        transmit = None
        prefix = [None] * 3
        before = [None] * 3
        for i in range(samples - 1):
            after = cell(rows, 0, i + 1)
            opacity = opacity_of(here + after)
            here = after
            if i == 0:
                weight = opacity
                transmit = 1.0 - opacity
            else:
                weight = transmit * opacity
                transmit = transmit - weight
            for c in range(3):
                next_color = cell(planes, c, i + 1)
                color = color_here[c] + next_color
                color_here[c] = next_color
                seen = weight * color
                prefix[c] = seen if i == 0 else prefix[c] + seen
                value = transmit * color + prefix[c]
                if i == 0:
                    out_first[c, part] = value
                else:
                    out_h[g, c, i - 1] = value + before[c]
                before[c] = value
        out_state[0, part] = transmit
        for c in range(3):
            out_state[1 + c, part] = prefix[c]
            out_last[c, part] = before[c]
            to_core[c, part] = jnp.where(even, color_here[c], color_first[c])
            to_chip[c, part] = jnp.where(even, color_first[c], color_here[c])


def boundary_kernel(
    own_core, own_chip, rim_core, rim_chip, core_colors, chip_colors, state, mine, other, out_opacity, full
):
    blocks = state.shape[1]
    half = blocks // 2
    index = lax.axis_index("depth")
    parity = lax.rem(index, 2)
    even = parity == 0
    for at in range(0, blocks, BLOCKS):
        part = pl.ds(at, BLOCKS)
        of_core = opacity_of(own_core[0, part] + rim_core[0, part])
        ends = index == lax.axis_size("depth") - 1
        of_chip = opacity_of(own_chip[0, part] + jnp.where(ends, 0.0, rim_chip[0, part]))
        ahead = jnp.where(index == 0, 0.0, jnp.where(even, of_chip, of_core))
        behind = jnp.where(even, of_core, of_chip)
        out_opacity[0, part] = ahead
        through = 1.0 - ahead
        transmit = through * state[0, part]
        full[0, part] = transmit
        closing = transmit * behind
        for c in range(3):
            first = jnp.where(even, chip_colors[c, part], core_colors[c, part])
            last = jnp.where(even, core_colors[c, part], chip_colors[c, part])
            full[1 + c, part] = ahead * first + through * state[1 + c, part] + closing * last
    mine[...] = full[:, pl.ds(pl.multiple_of(parity * half, SUB), half), :]
    other[...] = full[:, pl.ds(pl.multiple_of((1 - parity) * half, SUB), half), :]


def grad_kernel(
    halves, groups, mine, theirs, h, first, last, state, opacity, own_core, own_chip, *refs
):
    out, buffers, sems = refs[-3:]
    edges = 0 in groups
    if edges:
        rim_core, rim_chip = refs[:2]
    tiles, blocks = out.shape[0], out.shape[1]
    samples = tiles * SUB
    half = blocks // 2
    step = BLOCKS
    index = lax.axis_index("depth")
    parity = lax.rem(index, 2)
    even = parity == 0
    count = half // step

    def copies(which, k):
        start = pl.multiple_of((parity if which == 0 else 1 - parity) * half, step)
        part = pl.ds(pl.multiple_of(start + k * step, step), step)
        return [
            pltpu.make_async_copy(
                buffers.at[at, k, place], out.at[group, part], sems.at[at, k, place]
            )
            for at, whose in enumerate(halves)
            if whose == which
            for place, group in enumerate(groups)
        ]

    def piece(which, k):
        start = pl.multiple_of((parity if which == 0 else 1 - parity) * half, step)
        inside = pl.multiple_of(k * step, step)
        part = pl.ds(pl.multiple_of(start + k * step, step), step)
        slot = lax.div(start, step) + k
        if which == 0:
            a0, a1, a2, base = (mine[c, pl.ds(inside, step)] for c in range(4))
        else:
            a0, a1, a2, base = (theirs[pl.ds(c * half + inside, step), :] for c in range(4))
        ahead = opacity[0, part]
        core = [own_core[c, part] for c in range(3)]
        chip = [own_chip[c, part] for c in range(3)]
        opening = [jnp.where(even, chip[c], core[c]) for c in range(3)]
        base = base - 2.0 * ahead * (a0 * opening[0] + a1 * opening[1] + a2 * opening[2])
        through = 1.0 - ahead
        a0, a1, a2 = through * a0, through * a1, through * a2
        if edges:
            of_core = [core[c] + rim_core[c, part] for c in range(3)]
            ends = index == lax.axis_size("depth") - 1
            of_chip = [chip[c] + jnp.where(ends, 0.0, rim_chip[c, part]) for c in range(3)]
        for place, group in enumerate(groups):
            rows = buffers.at[halves.index(which), k, place].reshape(step * SUB, LANES)
            for i in range(group * SUB, (group + 1) * SUB):
                away = base
                if i == 0:
                    h0, h1, h2 = (
                        first[c, part]
                        + jnp.where(index == 0, 0.0, jnp.where(even, of_chip[c], of_core[c]))
                        for c in range(3)
                    )
                    away = jnp.where(index == 0, 0.5 * base, base)
                elif i == samples - 1:
                    h0, h1, h2 = (
                        last[c, part]
                        + state[1 + c, part]
                        + state[0, part] * jnp.where(even, of_core[c], of_chip[c])
                        for c in range(3)
                    )
                else:
                    h0, h1, h2 = (h[slot, c, i - 1] for c in range(3))
                value = a0 * h0 + a1 * h1 + a2 * h2 - away
                rows[pl.ds(i % SUB, step, stride=SUB), :] = value
        for copy in copies(which, k):
            copy.start()

    for which in halves:
        pl.loop(0, count)(functools.partial(piece, which))

    @pl.loop(0, count)
    def _(k):
        for which in halves:
            for copy in copies(which, k):
                copy.wait()


def sent(value, axis, pairs):
    return lax.ppermute(value, axis, pairs)


def compose(front, back):
    return [front[0] * back[0]] + [front[c] + front[0] * back[c] for c in range(1, 4)]


def chosen(flag, yes, no):
    return [jnp.where(flag, a, b) for a, b in zip(yes, no, strict=True)]


def chip_kernel(mine, theirs, out):
    even = lax.rem(lax.axis_index("depth"), 2) == 0
    for at in range(0, out.shape[1], BLOCKS):
        part = pl.ds(at, BLOCKS)
        own = [mine[c, part] for c in range(4)]
        far = [theirs[c, part] for c in range(4)]
        total = compose(chosen(even, own, far), chosen(even, far, own))
        for c in range(4):
            out[c, part] = total[c]


def gathered(members, earlier, part, stride):
    width = len(members)
    digit = lax.rem(lax.div(lax.axis_index("depth"), stride), width)
    values = [[member[c, part] for c in range(4)] for member in members]
    ordered = []
    for place in range(width):
        picked = values[0]
        for k in range(1, width):
            source = digit ^ k if width & (width - 1) == 0 else lax.rem(digit + k, width)
            picked = chosen(source == place, values[k], picked)
        ordered.append(picked)
    one = jnp.ones_like(values[0][0])
    ahead = [one] + [jnp.zeros_like(one)] * 3
    total = ordered[0]
    for place in range(1, width):
        ahead = chosen(digit == place, total, ahead)
        total = compose(total, ordered[place])
    if earlier is not None:
        ahead = compose(ahead, [earlier[c, part] for c in range(4)])
    return ahead, total


def stage_kernel(stride, width, started, *refs):
    members = refs[:width]
    earlier = refs[width] if started else None
    out_ahead, out_total = refs[-2:]
    for at in range(0, out_total.shape[1], BLOCKS):
        part = pl.ds(at, BLOCKS)
        ahead, total = gathered(members, earlier, part, stride)
        for c in range(4):
            out_ahead[c, part] = ahead[c]
            out_total[c, part] = total[c]


def scale_kernel(stride, width, started, mine, theirs, target, *refs):
    members = refs[:width]
    earlier = refs[width] if started else None
    out_mine, out_other, out_loss = refs[-3:]
    half = out_mine.shape[1]
    parity = lax.rem(lax.axis_index("depth"), 2)
    even = parity == 0
    loss = None
    for at in range(0, half, BLOCKS):
        part = pl.ds(at, BLOCKS)
        before, total = gathered(members, earlier, part, stride)
        own = [mine[c, part] for c in range(4)]
        far = [theirs[c, part] for c in range(4)]
        behind = compose(before, chosen(even, own, far))
        goal = pl.ds(pl.multiple_of(parity * half + at, SUB), BLOCKS)
        error = [0.5 * total[c] - target[c - 1, goal] for c in range(1, 4)]
        squares = error[0] * error[0] + error[1] * error[1] + error[2] * error[2]
        loss = squares if loss is None else loss + squares
        for ahead, is_own in ((before, even), (behind, jnp.logical_not(even))):
            gain = 0.5 * ahead[0]
            values = [gain * error[c] for c in range(3)]
            base = error[0] * (total[1] - ahead[1])
            for c in (1, 2):
                base = base + error[c] * (total[1 + c] - ahead[1 + c])
            values.append(base)

            @pl.when(is_own)
            def _():
                for c in range(4):
                    out_mine[c, part] = values[c]

            @pl.when(jnp.logical_not(is_own))
            def _():
                for c in range(4):
                    out_other[pl.ds(c * half + at, BLOCKS), :] = values[c]

    loss = jnp.full((SUB, LANES), jnp.sum(loss), jnp.float32)
    out_other[pl.ds(4 * half, SUB), :] = loss
    out_loss[...] = loss


def stages(count):
    while count > 1:
        width = 4 if count % 4 == 0 else 2 if count % 2 == 0 else count
        yield width
        count //= width


def ring_sum(count):
    if count & (count - 1) == 0 and count > 1:
        steps = [1 << bit for bit in range(count.bit_length() - 1)]
        return [[[(d, d ^ step) for d in range(count)]] for step in steps]
    return [[[(d, (d + k) % count) for d in range(count)] for k in range(1, count)]]


def partner(device, stride, width, step):
    digit = device // stride % width
    source = digit ^ step if width & (width - 1) == 0 else (digit + step) % width
    return device + (source - digit) * stride


def on_device(density, radiance, target):
    samples, ray_count = density.shape
    devices = lax.axis_size("depth")
    tiles, blocks = samples // SUB, ray_count // LANES
    half = blocks // 2
    f32 = jnp.float32

    def tiled(value):
        lead = value.shape[:-2]
        value = value.reshape(lead + (tiles, SUB, blocks, LANES))
        return jnp.swapaxes(value, -3, -2)

    density = tiled(density)
    radiance = tiled(radiance)
    swap = [(d, d ^ 1) for d in range(devices)]

    row = jax.ShapeDtypeStruct((1, blocks, LANES), f32)
    colors = jax.ShapeDtypeStruct((3, blocks, LANES), f32)
    states = jax.ShapeDtypeStruct((4, blocks, LANES), f32)
    whole = pl.BlockSpec(memory_space=pltpu.VMEM)
    stays = pl.BlockSpec(memory_space=pl.ANY)
    chain = [p for d in range(1, devices - 1, 2) for p in ((d, d + 1), (d + 1, d))]
    chain += [(0, devices - 1), (devices - 1, 0)]
    core_cell, chip_cell = pl.pallas_call(
        edge_kernel,
        out_shape=(row, row),
        in_specs=[stays, stays],
        out_specs=(whole, whole),
        scratch_shapes=[pltpu.VMEM((2, blocks, LANES), f32), pltpu.SemaphoreType.DMA((2,))],
        compiler_params=pltpu.CompilerParams(vmem_limit_bytes=EDGES),
        name="edge",
    )(density, radiance)
    rim_chip = sent(chip_cell, "depth", chain)
    rim_core = sent(core_cell, "depth", swap)

    step = BLOCKS
    grid = blocks // step
    h, state, first, last, core_colors, chip_colors = pl.pallas_call(
        slab_kernel,
        out_shape=(
            jax.ShapeDtypeStruct((grid, 3, samples - 2, step, LANES), f32),
            states,
            colors,
            colors,
            colors,
            colors,
        ),
        in_specs=[whole, whole],
        out_specs=(whole,) * 6,
        compiler_params=pltpu.CompilerParams(vmem_limit_bytes=KEPT),
        cost_estimate=pl.CostEstimate(
            flops=40 * samples * ray_count,
            bytes_accessed=16 * samples * ray_count,
            transcendentals=0,
        ),
        name="slab",
    )(density, radiance)

    part = jax.ShapeDtypeStruct((4, half, LANES), f32)
    edge_core = sent(core_colors, "depth", swap)
    edge_chip = sent(chip_colors, "depth", chain)
    mine, other, opacity = pl.pallas_call(
        boundary_kernel,
        out_shape=(part, part, row),
        in_specs=[whole] * 7,
        out_specs=(whole,) * 3,
        scratch_shapes=[pltpu.VMEM((4, blocks, LANES), f32)],
        compiler_params=pltpu.CompilerParams(vmem_limit_bytes=KEPT),
        name="boundary",
    )(core_cell, chip_cell, rim_core, rim_chip, core_colors, chip_colors, state)

    small = pltpu.CompilerParams(vmem_limit_bytes=SMALL)
    theirs = sent(other, "depth", swap)
    total = pl.pallas_call(
        chip_kernel,
        out_shape=part,
        in_specs=[whole, whole],
        out_specs=whole,
        compiler_params=small,
        name="chip",
    )(mine, theirs)
    goal = target.reshape(3, blocks, LANES)
    earlier = ()
    stride = 2
    widths = list(stages(devices // 2)) or [1]
    for at, width in enumerate(widths):
        members = [total] + [
            sent(total, "depth", [(partner(d, stride, width, k), d) for d in range(devices)])
            for k in range(1, width)
        ]
        last_stage = at == len(widths) - 1
        if last_stage:
            body = functools.partial(scale_kernel, stride, width, bool(earlier))
            given = (mine, theirs, goal, *members, *earlier)
            made = (
                part,
                jax.ShapeDtypeStruct((4 * half + SUB, LANES), f32),
                jax.ShapeDtypeStruct((SUB, LANES), f32),
            )
        else:
            body = functools.partial(stage_kernel, stride, width, bool(earlier))
            given = (*members, *earlier)
            made = (part, part)
        results = pl.pallas_call(
            body,
            out_shape=made,
            in_specs=[whole] * len(given),
            out_specs=(whole,) * len(made),
            compiler_params=small,
            name="scale" if last_stage else "stage",
        )(*given)
        if not last_stage:
            earlier, total = (results[0],), results[1]
        stride *= width
    scale_mine, scale_other, loss = results

    def grad_part(halves, chosen_tiles, *extra):
        given = (scale_mine, theirs, h, first, last, state, opacity, core_colors, chip_colors)
        if 0 in chosen_tiles:
            given += (edge_core, edge_chip)
        shape = (len(halves), grid // 2, len(chosen_tiles))
        share = math.prod(shape)
        return pl.pallas_call(
            functools.partial(grad_kernel, halves, chosen_tiles),
            out_shape=jax.ShapeDtypeStruct((tiles, blocks, SUB, LANES), f32),
            in_specs=[whole] * len(given) + [stays] * len(extra),
            out_specs=stays,
            input_output_aliases={len(given): 0} if extra else {},
            scratch_shapes=[
                pltpu.VMEM(shape + (step, SUB, LANES), f32),
                pltpu.SemaphoreType.DMA(shape),
            ],
            compiler_params=pltpu.CompilerParams(vmem_limit_bytes=KEPT),
            cost_estimate=pl.CostEstimate(
                flops=8 * share * step * SUB * LANES,
                bytes_accessed=16 * share * step * SUB * LANES,
                transcendentals=0,
            ),
            name="grad",
        )(*given, *extra)

    theirs = sent(scale_other, "depth", swap)
    groups = lax.axis_size("rays")
    rounds = ring_sum(groups)
    outer_tiles = tuple(sorted({0, tiles - 1}))
    inner_tiles = tuple(range(1, tiles - 1))
    grad = ()
    loss = loss + theirs[4 * half :]
    for pairs in rounds:
        others = [sent(loss, "rays", pair) for pair in pairs]
        loss = sum(others, loss)
    if inner_tiles:
        grad = (grad_part((0, 1), inner_tiles),)
    grad = grad_part((0, 1), outer_tiles, *grad)
    grad = jnp.swapaxes(grad, 1, 2).reshape(samples, ray_count)
    return grad, loss[0, 0] / (3.0 * ray_count * groups)


def solution(mesh):
    in_specs = (P("depth", "rays"), P(None, "depth", "rays"), P(None, "rays"))
    out_specs = (P("depth", "rays"), P())
    return jax.shard_map(
        on_device, mesh=mesh, in_specs=in_specs, out_specs=out_specs, check_vma=False
    )
```

```python
import functools
import math

import jax
import jax.numpy as jnp
from jax import lax
from jax.experimental import pallas as pl
from jax.experimental.pallas import tpu as pltpu
from jax.sharding import PartitionSpec as P


SUB = 8
LANES = 128
BLOCKS = 16
EDGES = 52 << 20
KEPT = 20 << 20
SMALL = 8 << 20

OPACITY = (
    0.49999998698510023,
    -0.12499944339862339,
    0.020829460991082075,
    -0.0025942459011451765,
    0.00024876881447613667,
    -1.5181374461261048e-05,
)


def opacity_of(pair):
    value = OPACITY[-1]
    for factor in OPACITY[-2::-1]:
        value = value * pair + factor
    return value * pair


def is_even():
    return lax.rem(lax.axis_index("depth"), 2) == 0


def edge_kernel(density, unused, to_core, to_chip, rows, sems):
    tiles = density.shape[0]
    first = pltpu.make_async_copy(density.at[0, :, 0, :], rows.at[0], sems.at[0])
    last = pltpu.make_async_copy(density.at[tiles - 1, :, SUB - 1, :], rows.at[1], sems.at[1])
    first.start()
    last.start()
    first.wait()
    last.wait()
    even = is_even()
    to_core[0] = jnp.where(even, rows[1], rows[0])
    to_chip[0] = jnp.where(even, rows[0], rows[1])


def opacity_kernel(density, out):
    tiles, blocks = density.shape[0], density.shape[1]
    rows = density.reshape(tiles * blocks * SUB, LANES)

    @pl.loop(0, blocks // BLOCKS)
    def _(g):
        def cell(i):
            base = pl.multiple_of(g * (BLOCKS * SUB), SUB) + (i // SUB) * blocks * SUB + i % SUB
            return rows[pl.ds(base, BLOCKS, stride=SUB), :]

        here = cell(0)
        for i in range(tiles * SUB - 1):
            after = cell(i + 1)
            out[g, i] = opacity_of(here + after)
            here = after


def slab_kernel(opacities, radiance, out_g, out_state, to_core, to_chip):
    tiles, blocks = radiance.shape[1], radiance.shape[2]
    samples = tiles * SUB
    step = BLOCKS
    planes = radiance.reshape(3 * tiles * blocks * SUB, LANES)
    even = is_even()

    @pl.loop(0, blocks // step)
    def _(g):
        part = pl.ds(pl.multiple_of(g * step, step), step)

        def color_of(c, i):
            base = (c * tiles + i // SUB) * blocks * SUB + i % SUB
            base = pl.multiple_of(g * (step * SUB), SUB) + base
            return planes[pl.ds(base, step, stride=SUB), :]

        color_here = [color_of(c, 0) for c in range(3)]
        color_first = list(color_here)
        transmit = None
        prefix = [None] * 3
        for i in range(samples - 1):
            opacity = opacities[g, i]
            if i == 0:
                weight = opacity
                transmit = 1.0 - opacity
            else:
                weight = transmit * opacity
                transmit = transmit - weight
            for c in range(3):
                next_color = color_of(c, i + 1)
                color = color_here[c] + next_color
                color_here[c] = next_color
                seen = weight * color
                prefix[c] = seen if i == 0 else prefix[c] + seen
                out_g[g, c, i] = transmit * color + prefix[c]
        out_state[0, part] = transmit
        for c in range(3):
            out_state[1 + c, part] = prefix[c]
            to_core[c, part] = jnp.where(even, color_here[c], color_first[c])
            to_chip[c, part] = jnp.where(even, color_first[c], color_here[c])


def boundary_kernel(
    own_core, own_chip, rim_core, rim_chip, core_colors, chip_colors, state, mine, other, out_opacity, full
):
    blocks = state.shape[1]
    half = blocks // 2
    index = lax.axis_index("depth")
    parity = lax.rem(index, 2)
    even = parity == 0
    for at in range(0, blocks, BLOCKS):
        part = pl.ds(at, BLOCKS)
        of_core = opacity_of(own_core[0, part] + rim_core[0, part])
        ends = index == lax.axis_size("depth") - 1
        of_chip = opacity_of(own_chip[0, part] + jnp.where(ends, 0.0, rim_chip[0, part]))
        ahead = jnp.where(index == 0, 0.0, jnp.where(even, of_chip, of_core))
        behind = jnp.where(even, of_core, of_chip)
        out_opacity[0, part] = ahead
        through = 1.0 - ahead
        transmit = through * state[0, part]
        full[0, part] = transmit
        closing = transmit * behind
        for c in range(3):
            first = jnp.where(even, chip_colors[c, part], core_colors[c, part])
            last = jnp.where(even, core_colors[c, part], chip_colors[c, part])
            full[1 + c, part] = ahead * first + through * state[1 + c, part] + closing * last
    mine[...] = full[:, pl.ds(pl.multiple_of(parity * half, SUB), half), :]
    other[...] = full[:, pl.ds(pl.multiple_of((1 - parity) * half, SUB), half), :]


def ends_kernel(mine, theirs, state, opacity, own_core, own_chip, gains, to_core, to_chip):
    half = mine.shape[1]
    parity = lax.rem(lax.axis_index("depth"), 2)
    even = parity == 0
    for scales, place in ((mine, parity), (theirs, 1 - parity)):
        for at in range(0, half, BLOCKS):
            inside = pl.ds(at, BLOCKS)
            part = pl.ds(pl.multiple_of(place * half + at, SUB), BLOCKS)
            ahead = opacity[0, part]
            through = 1.0 - ahead
            first = last = 0.0
            for c in range(3):
                scale = scales[c, inside]
                core, chip = own_core[c, part], own_chip[c, part]
                first = first + scale * jnp.where(even, chip, core)
                scale = through * scale
                last = last + scale * jnp.where(even, core, chip)
                gains[c, part] = scale
            gains[3, part] = 0.5 * scales[3, inside] - ahead * first
            last = state[0, part] * last
            to_core[0, part] = jnp.where(even, last, first)
            to_chip[0, part] = jnp.where(even, first, last)


def mean_kernel(scale, *refs):
    total = sum(ref[0, 0] for ref in refs[:-1])
    refs[-1][0, 0] = total * scale


def grad_kernel(groups, gains, values, *refs):
    out, buffers, sems = refs[-3:]
    if 0 in groups:
        state, opacity, own_core, own_chip, rim_core, rim_chip = refs[:6]
    tiles, blocks = out.shape[0], out.shape[1]
    samples = tiles * SUB
    step = BLOCKS
    index = lax.axis_index("depth")
    even = lax.rem(index, 2) == 0
    ends = index == lax.axis_size("depth") - 1
    count = blocks // step

    def copies(k):
        part = pl.ds(pl.multiple_of(k * step, step), step)
        return [
            pltpu.make_async_copy(buffers.at[k, place], out.at[group, part], sems.at[k, place])
            for place, group in enumerate(groups)
        ]

    @pl.loop(0, count)
    def _(k):
        part = pl.ds(pl.multiple_of(k * step, step), step)
        a0, a1, a2, base = (gains[c, part] for c in range(4))

        def sample(i):
            if i < 0:
                ahead = jnp.where(
                    even, own_chip[0, part] + rim_chip[0, part], own_core[0, part] + rim_core[0, part]
                )
                return jnp.where(index == 0, 0.0, (1.0 - opacity[0, part]) * ahead - base)
            if i < samples - 1:
                v0, v1, v2 = (values[k, c, i] for c in range(3))
                return a0 * v0 + a1 * v1 + a2 * v2 - base
            behind = jnp.where(
                even,
                own_core[0, part] + rim_core[0, part],
                own_chip[0, part] + jnp.where(ends, 0.0, rim_chip[0, part]),
            )
            v0, v1, v2 = (state[1 + c, part] for c in range(3))
            return a0 * v0 + a1 * v1 + a2 * v2 + behind - base

        for place, group in enumerate(groups):
            rows = buffers.at[k, place].reshape(step * SUB, LANES)
            if place == 0 or groups[place - 1] != group - 1:
                before = sample(group * SUB - 1)
            for i in range(group * SUB, (group + 1) * SUB):
                here = sample(i)
                rows[pl.ds(i % SUB, step, stride=SUB), :] = here + before
                before = here
        for copy in copies(k):
            copy.start()

    @pl.loop(0, count)
    def _(k):
        for copy in copies(k):
            copy.wait()


def sent(value, axis, pairs):
    return lax.ppermute(value, axis, pairs)


def compose(front, back):
    return [front[0] * back[0]] + [front[c] + front[0] * back[c] for c in range(1, 4)]


def chosen(flag, yes, no):
    return [jnp.where(flag, a, b) for a, b in zip(yes, no, strict=True)]


def chip_kernel(mine, theirs, out):
    even = lax.rem(lax.axis_index("depth"), 2) == 0
    for at in range(0, out.shape[1], BLOCKS):
        part = pl.ds(at, BLOCKS)
        own = [mine[c, part] for c in range(4)]
        far = [theirs[c, part] for c in range(4)]
        total = compose(chosen(even, own, far), chosen(even, far, own))
        for c in range(4):
            out[c, part] = total[c]


def gathered(members, earlier, part, stride):
    width = len(members)
    digit = lax.rem(lax.div(lax.axis_index("depth"), stride), width)
    values = [[member[c, part] for c in range(4)] for member in members]
    ordered = []
    for place in range(width):
        picked = values[0]
        for k in range(1, width):
            source = digit ^ k if width & (width - 1) == 0 else lax.rem(digit + k, width)
            picked = chosen(source == place, values[k], picked)
        ordered.append(picked)
    one = jnp.ones_like(values[0][0])
    ahead = [one] + [jnp.zeros_like(one)] * 3
    total = ordered[0]
    for place in range(1, width):
        ahead = chosen(digit == place, total, ahead)
        total = compose(total, ordered[place])
    if earlier is not None:
        ahead = compose(ahead, [earlier[c, part] for c in range(4)])
    return ahead, total


def stage_kernel(stride, width, started, *refs):
    members = refs[:width]
    earlier = refs[width] if started else None
    out_ahead, out_total = refs[-2:]
    for at in range(0, out_total.shape[1], BLOCKS):
        part = pl.ds(at, BLOCKS)
        ahead, total = gathered(members, earlier, part, stride)
        for c in range(4):
            out_ahead[c, part] = ahead[c]
            out_total[c, part] = total[c]


def scale_kernel(stride, width, started, mine, theirs, target, *refs):
    members = refs[:width]
    earlier = refs[width] if started else None
    out_mine, out_other, out_loss = refs[-3:]
    half = out_mine.shape[1]
    parity = lax.rem(lax.axis_index("depth"), 2)
    even = parity == 0
    loss = None
    for at in range(0, half, BLOCKS):
        part = pl.ds(at, BLOCKS)
        before, total = gathered(members, earlier, part, stride)
        own = [mine[c, part] for c in range(4)]
        far = [theirs[c, part] for c in range(4)]
        behind = compose(before, chosen(even, own, far))
        goal = pl.ds(pl.multiple_of(parity * half + at, SUB), BLOCKS)
        error = [0.5 * total[c] - target[c - 1, goal] for c in range(1, 4)]
        squares = error[0] * error[0] + error[1] * error[1] + error[2] * error[2]
        loss = squares if loss is None else loss + squares
        for ahead, is_own in ((before, even), (behind, jnp.logical_not(even))):
            gain = 0.5 * ahead[0]
            values = [gain * error[c] for c in range(3)]
            base = error[0] * (total[1] - ahead[1])
            for c in (1, 2):
                base = base + error[c] * (total[1 + c] - ahead[1 + c])
            values.append(base)

            @pl.when(is_own)
            def _():
                for c in range(4):
                    out_mine[c, part] = values[c]

            @pl.when(jnp.logical_not(is_own))
            def _():
                for c in range(4):
                    out_other[c, part] = values[c]

    out_loss[...] = jnp.full(out_loss.shape, jnp.sum(loss), jnp.float32)


def stages(count):
    while count > 1:
        width = 4 if count % 4 == 0 else 2 if count % 2 == 0 else count
        yield width
        count //= width


def ring_sum(count):
    if count & (count - 1) == 0 and count > 1:
        steps = [1 << bit for bit in reversed(range(count.bit_length() - 1))]
        return [[[(d, d ^ step) for d in range(count)]] for step in steps]
    return [[[(d, (d + k) % count) for d in range(count)] for k in range(1, count)]]


def partner(device, stride, width, step):
    digit = device // stride % width
    source = digit ^ step if width & (width - 1) == 0 else (digit + step) % width
    return device + (source - digit) * stride


def on_device(density, radiance, target):
    samples, ray_count = density.shape
    devices = lax.axis_size("depth")
    tiles, blocks = samples // SUB, ray_count // LANES
    half = blocks // 2
    f32 = jnp.float32

    def tiled(value):
        lead = value.shape[:-2]
        value = value.reshape(lead + (tiles, SUB, blocks, LANES))
        return jnp.swapaxes(value, -3, -2)

    density = tiled(density)
    radiance = tiled(radiance)
    swap = [(d, d ^ 1) for d in range(devices)]

    row = jax.ShapeDtypeStruct((1, blocks, LANES), f32)
    colors = jax.ShapeDtypeStruct((3, blocks, LANES), f32)
    states = jax.ShapeDtypeStruct((4, blocks, LANES), f32)
    whole = pl.BlockSpec(memory_space=pltpu.VMEM)
    stays = pl.BlockSpec(memory_space=pl.ANY)
    chain = [p for d in range(1, devices - 1, 2) for p in ((d, d + 1), (d + 1, d))]
    chain += [(0, devices - 1), (devices - 1, 0)]
    core_cell, chip_cell = pl.pallas_call(
        edge_kernel,
        out_shape=(row, row),
        in_specs=[stays, stays],
        out_specs=(whole, whole),
        scratch_shapes=[pltpu.VMEM((2, blocks, LANES), f32), pltpu.SemaphoreType.DMA((2,))],
        compiler_params=pltpu.CompilerParams(vmem_limit_bytes=EDGES),
        name="edge",
    )(density, radiance)
    rim_chip = sent(chip_cell, "depth", chain)
    rim_core = sent(core_cell, "depth", swap)

    step = BLOCKS
    grid = blocks // step
    opacities = pl.pallas_call(
        opacity_kernel,
        out_shape=jax.ShapeDtypeStruct((grid, samples - 1, step, LANES), f32),
        in_specs=[whole],
        out_specs=whole,
        compiler_params=pltpu.CompilerParams(vmem_limit_bytes=KEPT),
        cost_estimate=pl.CostEstimate(
            flops=12 * samples * ray_count,
            bytes_accessed=8 * samples * ray_count,
            transcendentals=0,
        ),
        name="opacity",
    )(density)
    values, state, core_colors, chip_colors = pl.pallas_call(
        slab_kernel,
        out_shape=(
            jax.ShapeDtypeStruct((grid, 3, samples - 1, step, LANES), f32),
            states,
            colors,
            colors,
        ),
        in_specs=[whole, whole],
        out_specs=(whole,) * 4,
        compiler_params=pltpu.CompilerParams(vmem_limit_bytes=KEPT),
        cost_estimate=pl.CostEstimate(
            flops=28 * samples * ray_count,
            bytes_accessed=28 * samples * ray_count,
            transcendentals=0,
        ),
        name="slab",
    )(opacities, radiance)

    part = jax.ShapeDtypeStruct((4, half, LANES), f32)
    mine, other, opacity = pl.pallas_call(
        boundary_kernel,
        out_shape=(part, part, row),
        in_specs=[whole] * 7,
        out_specs=(whole,) * 3,
        scratch_shapes=[pltpu.VMEM((4, blocks, LANES), f32)],
        compiler_params=pltpu.CompilerParams(vmem_limit_bytes=KEPT),
        name="boundary",
    )(core_cell, chip_cell, rim_core, rim_chip, core_colors, chip_colors, state)

    small = pltpu.CompilerParams(vmem_limit_bytes=SMALL)
    theirs = sent(other, "depth", swap)
    total = pl.pallas_call(
        chip_kernel,
        out_shape=part,
        in_specs=[whole, whole],
        out_specs=whole,
        compiler_params=small,
        name="chip",
    )(mine, theirs)
    goal = target.reshape(3, blocks, LANES)
    earlier = ()
    stride = 2
    widths = list(stages(devices // 2)) or [1]
    for at, width in enumerate(widths):
        members = [total] + [
            sent(total, "depth", [(partner(d, stride, width, k), d) for d in range(devices)])
            for k in range(1, width)
        ]
        last_stage = at == len(widths) - 1
        if last_stage:
            body = functools.partial(scale_kernel, stride, width, bool(earlier))
            given = (mine, theirs, goal, *members, *earlier)
            made = (
                part,
                part,
                jax.ShapeDtypeStruct((SUB, LANES), f32),
            )
        else:
            body = functools.partial(stage_kernel, stride, width, bool(earlier))
            given = (*members, *earlier)
            made = (part, part)
        results = pl.pallas_call(
            body,
            out_shape=made,
            in_specs=[whole] * len(given),
            out_specs=(whole,) * len(made),
            compiler_params=small,
            name="scale" if last_stage else "stage",
        )(*given)
        if not last_stage:
            earlier, total = (results[0],), results[1]
        stride *= width
    scale_mine, scale_other, loss = results

    groups = lax.axis_size("rays")
    rounds = ring_sum(groups)

    def rays_sum(at, value):
        return sum((sent(value, "rays", pairs) for pairs in rounds[at]), value)

    theirs = sent(scale_other, "depth", swap)
    loss = rays_sum(0, loss)
    gains, core_end, chip_end = pl.pallas_call(
        ends_kernel,
        out_shape=(states, row, row),
        in_specs=[whole] * 6,
        out_specs=(whole,) * 3,
        compiler_params=small,
        name="ends",
    )(scale_mine, theirs, state, opacity, core_colors, chip_colors)
    rim_end_chip = sent(chip_end, "depth", chain)
    rim_end_core = sent(core_end, "depth", swap)

    def grad_part(chosen_tiles, *extra):
        given = (gains, values)
        if 0 in chosen_tiles:
            given += (state, opacity, core_end, chip_end, rim_end_core, rim_end_chip)
        shape = (grid, len(chosen_tiles))
        share = math.prod(shape)
        return pl.pallas_call(
            functools.partial(grad_kernel, chosen_tiles),
            out_shape=jax.ShapeDtypeStruct((tiles, blocks, SUB, LANES), f32),
            in_specs=[whole] * len(given) + [stays] * len(extra),
            out_specs=stays,
            input_output_aliases={len(given): 0} if extra else {},
            scratch_shapes=[
                pltpu.VMEM(shape + (step, SUB, LANES), f32),
                pltpu.SemaphoreType.DMA(shape),
            ],
            compiler_params=pltpu.CompilerParams(vmem_limit_bytes=KEPT),
            cost_estimate=pl.CostEstimate(
                flops=8 * share * step * SUB * LANES,
                bytes_accessed=16 * share * step * SUB * LANES,
                transcendentals=0,
            ),
            name="grad",
        )(*given, *extra)

    outer_tiles = tuple(sorted({0, tiles - 1}))
    inner_tiles = tuple(range(1, tiles - 1))
    grad = (grad_part(inner_tiles),) if inner_tiles else ()
    grad = grad_part(outer_tiles, *grad)
    loss = loss + sent(loss, "depth", swap)
    for at in range(1, len(rounds) - 1):
        loss = rays_sum(at, loss)
    squares = [loss]
    if len(rounds) > 1:
        squares += [sent(loss, "rays", pairs) for pairs in rounds[-1]]
    scale = 1.0 / (3.0 * ray_count * groups)
    mean = pl.pallas_call(
        functools.partial(mean_kernel, scale),
        out_shape=jax.ShapeDtypeStruct((1, 1), f32),
        in_specs=[whole] * len(squares),
        out_specs=pl.BlockSpec(memory_space=pltpu.SMEM),
        compiler_params=small,
        name="mean",
    )(*squares)
    grad = jnp.swapaxes(grad, 1, 2).reshape(samples, ray_count)
    return grad, mean[0, 0]


def solution(mesh):
    in_specs = (P("depth", "rays"), P(None, "depth", "rays"), P(None, "rays"))
    out_specs = (P("depth", "rays"), P())
    return jax.shard_map(
        on_device, mesh=mesh, in_specs=in_specs, out_specs=out_specs, check_vma=False
    )
```

```python
import functools
import math

import jax
import jax.numpy as jnp
from jax import lax
from jax.experimental import pallas as pl
from jax.experimental.pallas import tpu as pltpu
from jax.sharding import PartitionSpec as P


SUB = 8
LANES = 128
BLOCKS = 16
EDGES = 52 << 20
KEPT = 20 << 20
SMALL = 8 << 20

OPACITY = (
    0.49999998698510023,
    -0.12499944339862339,
    0.020829460991082075,
    -0.0025942459011451765,
    0.00024876881447613667,
    -1.5181374461261048e-05,
)


def opacity_of(pair):
    value = OPACITY[-1]
    for factor in OPACITY[-2::-1]:
        value = value * pair + factor
    return value * pair


def is_even():
    return lax.rem(lax.axis_index("depth"), 2) == 0


def edge_kernel(density, unused, to_core, to_chip, rows, sems):
    tiles = density.shape[0]
    first = pltpu.make_async_copy(density.at[0, :, 0, :], rows.at[0], sems.at[0])
    last = pltpu.make_async_copy(density.at[tiles - 1, :, SUB - 1, :], rows.at[1], sems.at[1])
    first.start()
    last.start()
    first.wait()
    last.wait()
    even = is_even()
    to_core[0] = jnp.where(even, rows[1], rows[0])
    to_chip[0] = jnp.where(even, rows[0], rows[1])


def opacity_kernel(density, out):
    tiles, blocks = density.shape[0], density.shape[1]
    rows = density.reshape(tiles * blocks * SUB, LANES)

    @pl.loop(0, blocks // BLOCKS)
    def _(g):
        def cell(i):
            base = pl.multiple_of(g * (BLOCKS * SUB), SUB) + (i // SUB) * blocks * SUB + i % SUB
            return rows[pl.ds(base, BLOCKS, stride=SUB), :]

        here = cell(0)
        for i in range(tiles * SUB - 1):
            after = cell(i + 1)
            out[g, i] = opacity_of(here + after)
            here = after


def slab_kernel(opacities, radiance, out_g, out_state, to_core, to_chip):
    tiles, blocks = radiance.shape[1], radiance.shape[2]
    samples = tiles * SUB
    step = BLOCKS
    planes = radiance.reshape(3 * tiles * blocks * SUB, LANES)
    even = is_even()

    @pl.loop(0, blocks // step)
    def _(g):
        part = pl.ds(pl.multiple_of(g * step, step), step)

        def color_of(c, i):
            base = (c * tiles + i // SUB) * blocks * SUB + i % SUB
            base = pl.multiple_of(g * (step * SUB), SUB) + base
            return planes[pl.ds(base, step, stride=SUB), :]

        color_here = [color_of(c, 0) for c in range(3)]
        color_first = list(color_here)
        transmit = None
        prefix = [None] * 3
        for i in range(samples - 1):
            opacity = opacities[g, i]
            if i == 0:
                weight = opacity
                transmit = 1.0 - opacity
            else:
                weight = transmit * opacity
                transmit = transmit - weight
            for c in range(3):
                next_color = color_of(c, i + 1)
                color = color_here[c] + next_color
                color_here[c] = next_color
                seen = weight * color
                prefix[c] = seen if i == 0 else prefix[c] + seen
                out_g[g, c, i] = transmit * color + prefix[c]
        out_state[0, part] = transmit
        for c in range(3):
            out_state[1 + c, part] = prefix[c]
            to_core[c, part] = jnp.where(even, color_here[c], color_first[c])
            to_chip[c, part] = jnp.where(even, color_first[c], color_here[c])


def boundary_kernel(
    own_core, own_chip, rim_core, rim_chip, core_colors, chip_colors, state, mine, other, out_opacity, full
):
    blocks = state.shape[1]
    half = blocks // 2
    index = lax.axis_index("depth")
    parity = lax.rem(index, 2)
    even = parity == 0
    for at in range(0, blocks, BLOCKS):
        part = pl.ds(at, BLOCKS)
        of_core = opacity_of(own_core[0, part] + rim_core[0, part])
        ends = index == lax.axis_size("depth") - 1
        of_chip = opacity_of(own_chip[0, part] + jnp.where(ends, 0.0, rim_chip[0, part]))
        ahead = jnp.where(index == 0, 0.0, jnp.where(even, of_chip, of_core))
        behind = jnp.where(even, of_core, of_chip)
        out_opacity[0, part] = ahead
        through = 1.0 - ahead
        transmit = through * state[0, part]
        full[0, part] = transmit
        closing = transmit * behind
        for c in range(3):
            first = jnp.where(even, chip_colors[c, part], core_colors[c, part])
            last = jnp.where(even, core_colors[c, part], chip_colors[c, part])
            full[1 + c, part] = ahead * first + through * state[1 + c, part] + closing * last
    mine[...] = full[:, pl.ds(pl.multiple_of(parity * half, SUB), half), :]
    other[...] = full[:, pl.ds(pl.multiple_of((1 - parity) * half, SUB), half), :]


def ends_kernel(mine, theirs, state, opacity, own_core, own_chip, gains, to_core, to_chip):
    half = mine.shape[1]
    parity = lax.rem(lax.axis_index("depth"), 2)
    even = parity == 0
    for scales, place in ((mine, parity), (theirs, 1 - parity)):
        for at in range(0, half, BLOCKS):
            inside = pl.ds(at, BLOCKS)
            part = pl.ds(pl.multiple_of(place * half + at, SUB), BLOCKS)
            ahead = opacity[0, part]
            through = 1.0 - ahead
            first = last = 0.0
            for c in range(3):
                scale = scales[c, inside]
                core, chip = own_core[c, part], own_chip[c, part]
                first = first + scale * jnp.where(even, chip, core)
                scale = through * scale
                last = last + scale * jnp.where(even, core, chip)
                gains[c, part] = scale
            gains[3, part] = 0.5 * scales[3, inside] - ahead * first
            last = state[0, part] * last
            to_core[0, part] = jnp.where(even, last, first)
            to_chip[0, part] = jnp.where(even, first, last)


def mean_kernel(scale, *refs):
    total = sum(ref[:1, :1] for ref in refs[:-1])
    refs[-1][...] = total * scale


def grad_kernel(groups, gains, values, *refs):
    out, buffers, sems = refs[-3:]
    if 0 in groups:
        state, opacity, own_core, own_chip, rim_core, rim_chip = refs[:6]
    tiles, blocks = out.shape[0], out.shape[1]
    samples = tiles * SUB
    step = BLOCKS
    index = lax.axis_index("depth")
    even = lax.rem(index, 2) == 0
    ends = index == lax.axis_size("depth") - 1
    count = blocks // step

    def copies(k):
        part = pl.ds(pl.multiple_of(k * step, step), step)
        return [
            pltpu.make_async_copy(buffers.at[k, place], out.at[group, part], sems.at[k, place])
            for place, group in enumerate(groups)
        ]

    @pl.loop(0, count)
    def _(k):
        part = pl.ds(pl.multiple_of(k * step, step), step)
        a0, a1, a2, base = (gains[c, part] for c in range(4))

        def sample(i):
            if i < 0:
                ahead = jnp.where(
                    even, own_chip[0, part] + rim_chip[0, part], own_core[0, part] + rim_core[0, part]
                )
                return jnp.where(index == 0, 0.0, (1.0 - opacity[0, part]) * ahead - base)
            if i < samples - 1:
                v0, v1, v2 = (values[k, c, i] for c in range(3))
                return a0 * v0 + a1 * v1 + a2 * v2 - base
            behind = jnp.where(
                even,
                own_core[0, part] + rim_core[0, part],
                own_chip[0, part] + jnp.where(ends, 0.0, rim_chip[0, part]),
            )
            v0, v1, v2 = (state[1 + c, part] for c in range(3))
            return a0 * v0 + a1 * v1 + a2 * v2 + behind - base

        for place, group in enumerate(groups):
            rows = buffers.at[k, place].reshape(step * SUB, LANES)
            if place == 0 or groups[place - 1] != group - 1:
                before = sample(group * SUB - 1)
            for i in range(group * SUB, (group + 1) * SUB):
                here = sample(i)
                rows[pl.ds(i % SUB, step, stride=SUB), :] = here + before
                before = here
        for copy in copies(k):
            copy.start()

    @pl.loop(0, count)
    def _(k):
        for copy in copies(k):
            copy.wait()


def sent(value, axis, pairs):
    return lax.ppermute(value, axis, pairs)


def compose(front, back):
    return [front[0] * back[0]] + [front[c] + front[0] * back[c] for c in range(1, 4)]


def chosen(flag, yes, no):
    return [jnp.where(flag, a, b) for a, b in zip(yes, no, strict=True)]


def chip_kernel(mine, theirs, out):
    even = lax.rem(lax.axis_index("depth"), 2) == 0
    for at in range(0, out.shape[1], BLOCKS):
        part = pl.ds(at, BLOCKS)
        own = [mine[c, part] for c in range(4)]
        far = [theirs[c, part] for c in range(4)]
        total = compose(chosen(even, own, far), chosen(even, far, own))
        for c in range(4):
            out[c, part] = total[c]


def gathered(members, earlier, part, stride):
    width = len(members)
    digit = lax.rem(lax.div(lax.axis_index("depth"), stride), width)
    values = [[member[c, part] for c in range(4)] for member in members]
    ordered = []
    for place in range(width):
        picked = values[0]
        for k in range(1, width):
            source = digit ^ k if width & (width - 1) == 0 else lax.rem(digit + k, width)
            picked = chosen(source == place, values[k], picked)
        ordered.append(picked)
    one = jnp.ones_like(values[0][0])
    ahead = [one] + [jnp.zeros_like(one)] * 3
    total = ordered[0]
    for place in range(1, width):
        ahead = chosen(digit == place, total, ahead)
        total = compose(total, ordered[place])
    if earlier is not None:
        ahead = compose(ahead, [earlier[c, part] for c in range(4)])
    return ahead, total


def stage_kernel(stride, width, started, *refs):
    members = refs[:width]
    earlier = refs[width] if started else None
    out_ahead, out_total = refs[-2:]
    for at in range(0, out_total.shape[1], BLOCKS):
        part = pl.ds(at, BLOCKS)
        ahead, total = gathered(members, earlier, part, stride)
        for c in range(4):
            out_ahead[c, part] = ahead[c]
            out_total[c, part] = total[c]


def scale_kernel(stride, width, started, mine, theirs, target, *refs):
    members = refs[:width]
    earlier = refs[width] if started else None
    out_mine, out_other, out_loss = refs[-3:]
    half = out_mine.shape[1]
    parity = lax.rem(lax.axis_index("depth"), 2)
    even = parity == 0
    loss = None
    for at in range(0, half, BLOCKS):
        part = pl.ds(at, BLOCKS)
        before, total = gathered(members, earlier, part, stride)
        own = [mine[c, part] for c in range(4)]
        far = [theirs[c, part] for c in range(4)]
        behind = compose(before, chosen(even, own, far))
        goal = pl.ds(pl.multiple_of(parity * half + at, SUB), BLOCKS)
        error = [0.5 * total[c] - target[c - 1, goal] for c in range(1, 4)]
        squares = error[0] * error[0] + error[1] * error[1] + error[2] * error[2]
        loss = squares if loss is None else loss + squares
        for ahead, out in (
            (chosen(even, before, behind), out_mine),
            (chosen(even, behind, before), out_other),
        ):
            gain = 0.5 * ahead[0]
            for c in range(3):
                out[c, part] = gain * error[c]
            base = error[0] * (total[1] - ahead[1])
            for c in (1, 2):
                base = base + error[c] * (total[1 + c] - ahead[1 + c])
            out[3, part] = base

    out_loss[...] = jnp.full(out_loss.shape, jnp.sum(loss), jnp.float32)


def stages(count):
    while count > 1:
        width = 4 if count % 4 == 0 else 2 if count % 2 == 0 else count
        yield width
        count //= width


def ring_sum(count):
    if count & (count - 1) == 0 and count > 1:
        steps = [1 << bit for bit in range(count.bit_length() - 1)]
        return [[[(d, d ^ step) for d in range(count)]] for step in steps]
    return [[[(d, (d + k) % count) for d in range(count)] for k in range(1, count)]]


def partner(device, stride, width, step):
    digit = device // stride % width
    source = digit ^ step if width & (width - 1) == 0 else (digit + step) % width
    return device + (source - digit) * stride


def on_device(density, radiance, target):
    samples, ray_count = density.shape
    devices = lax.axis_size("depth")
    tiles, blocks = samples // SUB, ray_count // LANES
    half = blocks // 2
    f32 = jnp.float32

    def tiled(value):
        lead = value.shape[:-2]
        value = value.reshape(lead + (tiles, SUB, blocks, LANES))
        return jnp.swapaxes(value, -3, -2)

    density = tiled(density)
    radiance = tiled(radiance)
    swap = [(d, d ^ 1) for d in range(devices)]

    row = jax.ShapeDtypeStruct((1, blocks, LANES), f32)
    colors = jax.ShapeDtypeStruct((3, blocks, LANES), f32)
    states = jax.ShapeDtypeStruct((4, blocks, LANES), f32)
    whole = pl.BlockSpec(memory_space=pltpu.VMEM)
    stays = pl.BlockSpec(memory_space=pl.ANY)
    chain = [p for d in range(1, devices - 1, 2) for p in ((d, d + 1), (d + 1, d))]
    chain += [(0, devices - 1), (devices - 1, 0)]
    core_cell, chip_cell = pl.pallas_call(
        edge_kernel,
        out_shape=(row, row),
        in_specs=[stays, stays],
        out_specs=(whole, whole),
        scratch_shapes=[pltpu.VMEM((2, blocks, LANES), f32), pltpu.SemaphoreType.DMA((2,))],
        compiler_params=pltpu.CompilerParams(vmem_limit_bytes=EDGES),
        name="edge",
    )(density, radiance)
    rim_chip = sent(chip_cell, "depth", chain)
    rim_core = sent(core_cell, "depth", swap)

    step = BLOCKS
    grid = blocks // step
    opacities = pl.pallas_call(
        opacity_kernel,
        out_shape=jax.ShapeDtypeStruct((grid, samples - 1, step, LANES), f32),
        in_specs=[whole],
        out_specs=whole,
        compiler_params=pltpu.CompilerParams(vmem_limit_bytes=KEPT),
        cost_estimate=pl.CostEstimate(
            flops=12 * samples * ray_count,
            bytes_accessed=8 * samples * ray_count,
            transcendentals=0,
        ),
        name="opacity",
    )(density)
    values, state, core_colors, chip_colors = pl.pallas_call(
        slab_kernel,
        out_shape=(
            jax.ShapeDtypeStruct((grid, 3, samples - 1, step, LANES), f32),
            states,
            colors,
            colors,
        ),
        in_specs=[whole, whole],
        out_specs=(whole,) * 4,
        compiler_params=pltpu.CompilerParams(vmem_limit_bytes=KEPT),
        cost_estimate=pl.CostEstimate(
            flops=28 * samples * ray_count,
            bytes_accessed=28 * samples * ray_count,
            transcendentals=0,
        ),
        name="slab",
    )(opacities, radiance)

    part = jax.ShapeDtypeStruct((4, half, LANES), f32)
    mine, other, opacity = pl.pallas_call(
        boundary_kernel,
        out_shape=(part, part, row),
        in_specs=[whole] * 7,
        out_specs=(whole,) * 3,
        scratch_shapes=[pltpu.VMEM((4, blocks, LANES), f32)],
        compiler_params=pltpu.CompilerParams(vmem_limit_bytes=KEPT),
        name="boundary",
    )(core_cell, chip_cell, rim_core, rim_chip, core_colors, chip_colors, state)

    small = pltpu.CompilerParams(vmem_limit_bytes=SMALL)
    theirs = sent(other, "depth", swap)
    total = pl.pallas_call(
        chip_kernel,
        out_shape=part,
        in_specs=[whole, whole],
        out_specs=whole,
        compiler_params=small,
        name="chip",
    )(mine, theirs)
    goal = target.reshape(3, blocks, LANES)
    earlier = ()
    stride = 2
    widths = list(stages(devices // 2)) or [1]
    for at, width in enumerate(widths):
        members = [total] + [
            sent(total, "depth", [(partner(d, stride, width, k), d) for d in range(devices)])
            for k in range(1, width)
        ]
        last_stage = at == len(widths) - 1
        if last_stage:
            body = functools.partial(scale_kernel, stride, width, bool(earlier))
            given = (mine, theirs, goal, *members, *earlier)
            made = (
                part,
                part,
                jax.ShapeDtypeStruct((SUB, LANES), f32),
            )
        else:
            body = functools.partial(stage_kernel, stride, width, bool(earlier))
            given = (*members, *earlier)
            made = (part, part)
        results = pl.pallas_call(
            body,
            out_shape=made,
            in_specs=[whole] * len(given),
            out_specs=(whole,) * len(made),
            compiler_params=small,
            name="scale" if last_stage else "stage",
        )(*given)
        if not last_stage:
            earlier, total = (results[0],), results[1]
        stride *= width
    scale_mine, scale_other, loss = results

    groups = lax.axis_size("rays")
    rounds = ring_sum(groups)

    def rays_sum(at, value):
        return sum((sent(value, "rays", pairs) for pairs in rounds[at]), value)

    theirs = sent(scale_other, "depth", swap)
    loss = rays_sum(0, loss)
    gains, core_end, chip_end = pl.pallas_call(
        ends_kernel,
        out_shape=(states, row, row),
        in_specs=[whole] * 6,
        out_specs=(whole,) * 3,
        compiler_params=small,
        name="ends",
    )(scale_mine, theirs, state, opacity, core_colors, chip_colors)
    rim_end_chip = sent(chip_end, "depth", chain)
    rim_end_core = sent(core_end, "depth", swap)

    def grad_part(chosen_tiles, *extra):
        given = (gains, values)
        if 0 in chosen_tiles:
            given += (state, opacity, core_end, chip_end, rim_end_core, rim_end_chip)
        shape = (grid, len(chosen_tiles))
        share = math.prod(shape)
        return pl.pallas_call(
            functools.partial(grad_kernel, chosen_tiles),
            out_shape=jax.ShapeDtypeStruct((tiles, blocks, SUB, LANES), f32),
            in_specs=[whole] * len(given) + [stays] * len(extra),
            out_specs=stays,
            input_output_aliases={len(given): 0} if extra else {},
            scratch_shapes=[
                pltpu.VMEM(shape + (step, SUB, LANES), f32),
                pltpu.SemaphoreType.DMA(shape),
            ],
            compiler_params=pltpu.CompilerParams(vmem_limit_bytes=KEPT),
            cost_estimate=pl.CostEstimate(
                flops=8 * share * step * SUB * LANES,
                bytes_accessed=16 * share * step * SUB * LANES,
                transcendentals=0,
            ),
            name="grad",
        )(*given, *extra)

    outer_tiles = tuple(sorted({0, tiles - 1}))
    inner_tiles = tuple(range(1, tiles - 1))
    grad = (grad_part(inner_tiles),) if inner_tiles else ()
    grad = grad_part(outer_tiles, *grad)
    loss = loss + sent(loss, "depth", swap)
    for at in range(1, len(rounds) - 1):
        loss = rays_sum(at, loss)
    squares = [loss]
    if len(rounds) > 1:
        squares += [sent(loss, "rays", pairs) for pairs in rounds[-1]]
    scale = 1.0 / (3.0 * ray_count * groups)
    mean = pl.pallas_call(
        functools.partial(mean_kernel, scale),
        out_shape=jax.ShapeDtypeStruct((1, 1), f32),
        in_specs=[whole] * len(squares),
        out_specs=whole,
        compiler_params=small,
        name="mean",
    )(*squares)
    grad = jnp.swapaxes(grad, 1, 2).reshape(samples, ray_count)
    return grad, mean[0, 0]


def solution(mesh):
    in_specs = (P("depth", "rays"), P(None, "depth", "rays"), P(None, "rays"))
    out_specs = (P("depth", "rays"), P())
    return jax.shard_map(
        on_device, mesh=mesh, in_specs=in_specs, out_specs=out_specs, check_vma=False
    )
```

```python
import functools
import math

import jax
import jax.numpy as jnp
from jax import lax
from jax.experimental import pallas as pl
from jax.experimental.pallas import tpu as pltpu
from jax.sharding import PartitionSpec as P


SUB = 8
LANES = 128
BLOCKS = 16
EDGES = 52 << 20
KEPT = 20 << 20
SMALL = 8 << 20

OPACITY = (
    0.49999998698510023,
    -0.12499944339862339,
    0.020829460991082075,
    -0.0025942459011451765,
    0.00024876881447613667,
    -1.5181374461261048e-05,
)


def opacity_of(pair):
    value = OPACITY[-1]
    for factor in OPACITY[-2::-1]:
        value = value * pair + factor
    return value * pair


def is_even():
    return lax.rem(lax.axis_index("depth"), 2) == 0


def edge_kernel(density, unused, to_core, to_chip, rows, sems):
    tiles = density.shape[0]
    first = pltpu.make_async_copy(density.at[0, :, 0, :], rows.at[0], sems.at[0])
    last = pltpu.make_async_copy(density.at[tiles - 1, :, SUB - 1, :], rows.at[1], sems.at[1])
    first.start()
    last.start()
    first.wait()
    last.wait()
    even = is_even()
    to_core[0] = jnp.where(even, rows[1], rows[0])
    to_chip[0] = jnp.where(even, rows[0], rows[1])


def opacity_kernel(density, out):
    tiles, blocks = density.shape[0], density.shape[1]
    rows = density.reshape(tiles * blocks * SUB, LANES)

    @pl.loop(0, blocks // BLOCKS)
    def _(g):
        def cell(i):
            base = pl.multiple_of(g * (BLOCKS * SUB), SUB) + (i // SUB) * blocks * SUB + i % SUB
            return rows[pl.ds(base, BLOCKS, stride=SUB), :]

        here = cell(0)
        for i in range(tiles * SUB - 1):
            after = cell(i + 1)
            out[g, i] = opacity_of(here + after)
            here = after


def slab_kernel(opacities, radiance, out_g, out_state, to_core, to_chip):
    tiles, blocks = radiance.shape[1], radiance.shape[2]
    samples = tiles * SUB
    step = BLOCKS
    planes = radiance.reshape(3 * tiles * blocks * SUB, LANES)
    even = is_even()

    @pl.loop(0, blocks // step)
    def _(g):
        part = pl.ds(pl.multiple_of(g * step, step), step)

        def color_of(c, i):
            base = (c * tiles + i // SUB) * blocks * SUB + i % SUB
            base = pl.multiple_of(g * (step * SUB), SUB) + base
            return planes[pl.ds(base, step, stride=SUB), :]

        color_here = [color_of(c, 0) for c in range(3)]
        color_first = list(color_here)
        transmit = None
        prefix = [None] * 3
        for i in range(samples - 1):
            opacity = opacities[g, i]
            if i == 0:
                weight = opacity
                transmit = 1.0 - opacity
            else:
                weight = transmit * opacity
                transmit = transmit - weight
            for c in range(3):
                next_color = color_of(c, i + 1)
                color = color_here[c] + next_color
                color_here[c] = next_color
                seen = weight * color
                prefix[c] = seen if i == 0 else prefix[c] + seen
                out_g[g, c, i] = transmit * color + prefix[c]
        out_state[0, part] = transmit
        for c in range(3):
            out_state[1 + c, part] = prefix[c]
            to_core[c, part] = jnp.where(even, color_here[c], color_first[c])
            to_chip[c, part] = jnp.where(even, color_first[c], color_here[c])


def boundary_kernel(
    own_core, own_chip, rim_core, rim_chip, core_colors, chip_colors, state, mine, other, out_opacity, full
):
    blocks = state.shape[1]
    half = blocks // 2
    index = lax.axis_index("depth")
    parity = lax.rem(index, 2)
    even = parity == 0
    for at in range(0, blocks, BLOCKS):
        part = pl.ds(at, BLOCKS)
        of_core = opacity_of(own_core[0, part] + rim_core[0, part])
        ends = index == lax.axis_size("depth") - 1
        of_chip = opacity_of(own_chip[0, part] + jnp.where(ends, 0.0, rim_chip[0, part]))
        ahead = jnp.where(index == 0, 0.0, jnp.where(even, of_chip, of_core))
        behind = jnp.where(even, of_core, of_chip)
        out_opacity[0, part] = ahead
        through = 1.0 - ahead
        transmit = through * state[0, part]
        full[0, part] = transmit
        closing = transmit * behind
        for c in range(3):
            first = jnp.where(even, chip_colors[c, part], core_colors[c, part])
            last = jnp.where(even, core_colors[c, part], chip_colors[c, part])
            full[1 + c, part] = ahead * first + through * state[1 + c, part] + closing * last
    mine[...] = full[:, pl.ds(pl.multiple_of(parity * half, SUB), half), :]
    other[...] = full[:, pl.ds(pl.multiple_of((1 - parity) * half, SUB), half), :]


def ends_kernel(mine, theirs, state, opacity, own_core, own_chip, gains, to_core, to_chip):
    half = mine.shape[1]
    parity = lax.rem(lax.axis_index("depth"), 2)
    even = parity == 0
    for scales, place in ((mine, parity), (theirs, 1 - parity)):
        for at in range(0, half, BLOCKS):
            inside = pl.ds(at, BLOCKS)
            part = pl.ds(pl.multiple_of(place * half + at, SUB), BLOCKS)
            ahead = opacity[0, part]
            through = 1.0 - ahead
            first = last = 0.0
            for c in range(3):
                scale = scales[c, inside]
                core, chip = own_core[c, part], own_chip[c, part]
                first = first + scale * jnp.where(even, chip, core)
                scale = through * scale
                last = last + scale * jnp.where(even, core, chip)
                gains[c, part] = scale
            gains[3, part] = 0.5 * scales[3, inside] - ahead * first
            last = state[0, part] * last
            to_core[0, part] = jnp.where(even, last, first)
            to_chip[0, part] = jnp.where(even, first, last)


def mean_kernel(scale, *refs):
    total = sum(ref[:1, :1] for ref in refs[:-1])
    refs[-1][...] = total * scale


def grad_kernel(groups, gains, values, *refs):
    out, buffers, sems = refs[-3:]
    if 0 in groups:
        state, opacity, own_core, own_chip, rim_core, rim_chip = refs[:6]
    tiles, blocks = out.shape[0], out.shape[1]
    samples = tiles * SUB
    step = BLOCKS
    index = lax.axis_index("depth")
    even = lax.rem(index, 2) == 0
    ends = index == lax.axis_size("depth") - 1
    count = blocks // step

    def copies(k):
        part = pl.ds(pl.multiple_of(k * step, step), step)
        return [
            pltpu.make_async_copy(buffers.at[k, place], out.at[group, part], sems.at[k, place])
            for place, group in enumerate(groups)
        ]

    @pl.loop(0, count)
    def _(k):
        part = pl.ds(pl.multiple_of(k * step, step), step)
        a0, a1, a2, base = (gains[c, part] for c in range(4))

        def sample(i):
            if i < 0:
                ahead = jnp.where(
                    even, own_chip[0, part] + rim_chip[0, part], own_core[0, part] + rim_core[0, part]
                )
                return jnp.where(index == 0, 0.0, (1.0 - opacity[0, part]) * ahead - base)
            if i < samples - 1:
                v0, v1, v2 = (values[k, c, i] for c in range(3))
                return a0 * v0 + a1 * v1 + a2 * v2 - base
            behind = jnp.where(
                even,
                own_core[0, part] + rim_core[0, part],
                own_chip[0, part] + jnp.where(ends, 0.0, rim_chip[0, part]),
            )
            v0, v1, v2 = (state[1 + c, part] for c in range(3))
            return a0 * v0 + a1 * v1 + a2 * v2 + behind - base

        for place, group in enumerate(groups):
            rows = buffers.at[k, place].reshape(step * SUB, LANES)
            if place == 0 or groups[place - 1] != group - 1:
                before = sample(group * SUB - 1)
            for i in range(group * SUB, (group + 1) * SUB):
                here = sample(i)
                rows[pl.ds(i % SUB, step, stride=SUB), :] = here + before
                before = here
        for copy in copies(k):
            copy.start()

    @pl.loop(0, count)
    def _(k):
        for copy in copies(k):
            copy.wait()


def sent(value, axis, pairs):
    return lax.ppermute(value, axis, pairs)


def compose(front, back):
    return [front[0] * back[0]] + [front[c] + front[0] * back[c] for c in range(1, 4)]


def chosen(flag, yes, no):
    return [jnp.where(flag, a, b) for a, b in zip(yes, no, strict=True)]


def chip_kernel(mine, theirs, out):
    even = lax.rem(lax.axis_index("depth"), 2) == 0
    for at in range(0, out.shape[1], BLOCKS):
        part = pl.ds(at, BLOCKS)
        own = [mine[c, part] for c in range(4)]
        far = [theirs[c, part] for c in range(4)]
        total = compose(chosen(even, own, far), chosen(even, far, own))
        for c in range(4):
            out[c, part] = total[c]


def gathered(members, earlier, part, stride):
    width = len(members)
    digit = lax.rem(lax.div(lax.axis_index("depth"), stride), width)
    values = [[member[c, part] for c in range(4)] for member in members]
    ordered = []
    for place in range(width):
        picked = values[0]
        for k in range(1, width):
            source = digit ^ k if width & (width - 1) == 0 else lax.rem(digit + k, width)
            picked = chosen(source == place, values[k], picked)
        ordered.append(picked)
    one = jnp.ones_like(values[0][0])
    ahead = [one] + [jnp.zeros_like(one)] * 3
    total = ordered[0]
    for place in range(1, width):
        ahead = chosen(digit == place, total, ahead)
        total = compose(total, ordered[place])
    if earlier is not None:
        ahead = compose(ahead, [earlier[c, part] for c in range(4)])
    return ahead, total


def stage_kernel(stride, width, started, *refs):
    members = refs[:width]
    earlier = refs[width] if started else None
    out_ahead, out_total = refs[-2:]
    for at in range(0, out_total.shape[1], BLOCKS):
        part = pl.ds(at, BLOCKS)
        ahead, total = gathered(members, earlier, part, stride)
        for c in range(4):
            out_ahead[c, part] = ahead[c]
            out_total[c, part] = total[c]


def scale_kernel(stride, width, started, mine, theirs, target, *refs):
    members = refs[:width]
    earlier = refs[width] if started else None
    out_mine, out_other, out_loss = refs[-3:]
    half = out_mine.shape[1]
    parity = lax.rem(lax.axis_index("depth"), 2)
    even = parity == 0
    loss = None
    for at in range(0, half, BLOCKS):
        part = pl.ds(at, BLOCKS)
        before, total = gathered(members, earlier, part, stride)
        own = [mine[c, part] for c in range(4)]
        far = [theirs[c, part] for c in range(4)]
        behind = compose(before, chosen(even, own, far))
        goal = pl.ds(pl.multiple_of(parity * half + at, SUB), BLOCKS)
        error = [0.5 * total[c] - target[c - 1, goal] for c in range(1, 4)]
        squares = error[0] * error[0] + error[1] * error[1] + error[2] * error[2]
        loss = squares if loss is None else loss + squares
        for ahead, out in (
            (chosen(even, before, behind), out_mine),
            (chosen(even, behind, before), out_other),
        ):
            gain = 0.5 * ahead[0]
            for c in range(3):
                out[c, part] = gain * error[c]
            base = error[0] * (total[1] - ahead[1])
            for c in (1, 2):
                base = base + error[c] * (total[1 + c] - ahead[1 + c])
            out[3, part] = base

    out_loss[...] = jnp.full(out_loss.shape, jnp.sum(loss), jnp.float32)


def stages(count):
    while count > 1:
        width = 4 if count % 4 == 0 else 2 if count % 2 == 0 else count
        yield width
        count //= width


def ring_sum(count):
    if count & (count - 1) == 0 and count > 1:
        steps = [1 << bit for bit in range(count.bit_length() - 1)]
        return [[[(d, d ^ step) for d in range(count)]] for step in steps]
    return [[[(d, (d + k) % count) for d in range(count)] for k in range(1, count)]]


def partner(device, stride, width, step):
    digit = device // stride % width
    source = digit ^ step if width & (width - 1) == 0 else (digit + step) % width
    return device + (source - digit) * stride


def on_device(density, radiance, target):
    samples, ray_count = density.shape
    devices = lax.axis_size("depth")
    tiles, blocks = samples // SUB, ray_count // LANES
    half = blocks // 2
    f32 = jnp.float32

    def tiled(value):
        lead = value.shape[:-2]
        value = value.reshape(lead + (tiles, SUB, blocks, LANES))
        return jnp.swapaxes(value, -3, -2)

    density = tiled(density)
    radiance = tiled(radiance)
    swap = [(d, d ^ 1) for d in range(devices)]

    row = jax.ShapeDtypeStruct((1, blocks, LANES), f32)
    colors = jax.ShapeDtypeStruct((3, blocks, LANES), f32)
    states = jax.ShapeDtypeStruct((4, blocks, LANES), f32)
    whole = pl.BlockSpec(memory_space=pltpu.VMEM)
    stays = pl.BlockSpec(memory_space=pl.ANY)
    tiles_of_rays = lax.axis_size("rays")
    swaps = [p for d in range(1, devices - 1, 2) for p in ((d, d + 1), (d + 1, d))]
    chain = [
        (a * tiles_of_rays + z, b * tiles_of_rays + z) for a, b in swaps for z in range(tiles_of_rays)
    ]
    for end, far in ((0, devices - 1), (devices - 1, 0)):
        for z in range(tiles_of_rays):
            to, tile = (end, z ^ 1) if tiles_of_rays % 2 == 0 else (far, z)
            chain.append((end * tiles_of_rays + z, to * tiles_of_rays + tile))
    core_cell, chip_cell = pl.pallas_call(
        edge_kernel,
        out_shape=(row, row),
        in_specs=[stays, stays],
        out_specs=(whole, whole),
        scratch_shapes=[pltpu.VMEM((2, blocks, LANES), f32), pltpu.SemaphoreType.DMA((2,))],
        compiler_params=pltpu.CompilerParams(vmem_limit_bytes=EDGES),
        name="edge",
    )(density, radiance)
    rim_chip = sent(chip_cell, ("depth", "rays"), chain)
    rim_core = sent(core_cell, "depth", swap)

    step = BLOCKS
    grid = blocks // step
    opacities = pl.pallas_call(
        opacity_kernel,
        out_shape=jax.ShapeDtypeStruct((grid, samples - 1, step, LANES), f32),
        in_specs=[whole],
        out_specs=whole,
        compiler_params=pltpu.CompilerParams(vmem_limit_bytes=KEPT),
        cost_estimate=pl.CostEstimate(
            flops=12 * samples * ray_count,
            bytes_accessed=8 * samples * ray_count,
            transcendentals=0,
        ),
        name="opacity",
    )(density)
    values, state, core_colors, chip_colors = pl.pallas_call(
        slab_kernel,
        out_shape=(
            jax.ShapeDtypeStruct((grid, 3, samples - 1, step, LANES), f32),
            states,
            colors,
            colors,
        ),
        in_specs=[whole, whole],
        out_specs=(whole,) * 4,
        compiler_params=pltpu.CompilerParams(vmem_limit_bytes=KEPT),
        cost_estimate=pl.CostEstimate(
            flops=28 * samples * ray_count,
            bytes_accessed=28 * samples * ray_count,
            transcendentals=0,
        ),
        name="slab",
    )(opacities, radiance)

    part = jax.ShapeDtypeStruct((4, half, LANES), f32)
    mine, other, opacity = pl.pallas_call(
        boundary_kernel,
        out_shape=(part, part, row),
        in_specs=[whole] * 7,
        out_specs=(whole,) * 3,
        scratch_shapes=[pltpu.VMEM((4, blocks, LANES), f32)],
        compiler_params=pltpu.CompilerParams(vmem_limit_bytes=KEPT),
        name="boundary",
    )(core_cell, chip_cell, rim_core, rim_chip, core_colors, chip_colors, state)

    small = pltpu.CompilerParams(vmem_limit_bytes=SMALL)
    theirs = sent(other, "depth", swap)
    total = pl.pallas_call(
        chip_kernel,
        out_shape=part,
        in_specs=[whole, whole],
        out_specs=whole,
        compiler_params=small,
        name="chip",
    )(mine, theirs)
    goal = target.reshape(3, blocks, LANES)
    earlier = ()
    stride = 2
    widths = list(stages(devices // 2)) or [1]
    for at, width in enumerate(widths):
        members = [total] + [
            sent(total, "depth", [(partner(d, stride, width, k), d) for d in range(devices)])
            for k in range(1, width)
        ]
        last_stage = at == len(widths) - 1
        if last_stage:
            body = functools.partial(scale_kernel, stride, width, bool(earlier))
            given = (mine, theirs, goal, *members, *earlier)
            made = (
                part,
                part,
                jax.ShapeDtypeStruct((SUB, LANES), f32),
            )
        else:
            body = functools.partial(stage_kernel, stride, width, bool(earlier))
            given = (*members, *earlier)
            made = (part, part)
        results = pl.pallas_call(
            body,
            out_shape=made,
            in_specs=[whole] * len(given),
            out_specs=(whole,) * len(made),
            compiler_params=small,
            name="scale" if last_stage else "stage",
        )(*given)
        if not last_stage:
            earlier, total = (results[0],), results[1]
        stride *= width
    scale_mine, scale_other, loss = results

    groups = lax.axis_size("rays")
    rounds = ring_sum(groups)

    def rays_sum(at, value):
        return sum((sent(value, "rays", pairs) for pairs in rounds[at]), value)

    theirs = sent(scale_other, "depth", swap)
    loss = rays_sum(0, loss)
    gains, core_end, chip_end = pl.pallas_call(
        ends_kernel,
        out_shape=(states, row, row),
        in_specs=[whole] * 6,
        out_specs=(whole,) * 3,
        compiler_params=small,
        name="ends",
    )(scale_mine, theirs, state, opacity, core_colors, chip_colors)
    rim_end_chip = sent(chip_end, ("depth", "rays"), chain)
    rim_end_core = sent(core_end, "depth", swap)

    def grad_part(chosen_tiles, *extra):
        given = (gains, values)
        if 0 in chosen_tiles:
            given += (state, opacity, core_end, chip_end, rim_end_core, rim_end_chip)
        shape = (grid, len(chosen_tiles))
        share = math.prod(shape)
        return pl.pallas_call(
            functools.partial(grad_kernel, chosen_tiles),
            out_shape=jax.ShapeDtypeStruct((tiles, blocks, SUB, LANES), f32),
            in_specs=[whole] * len(given) + [stays] * len(extra),
            out_specs=stays,
            input_output_aliases={len(given): 0} if extra else {},
            scratch_shapes=[
                pltpu.VMEM(shape + (step, SUB, LANES), f32),
                pltpu.SemaphoreType.DMA(shape),
            ],
            compiler_params=pltpu.CompilerParams(vmem_limit_bytes=KEPT),
            cost_estimate=pl.CostEstimate(
                flops=8 * share * step * SUB * LANES,
                bytes_accessed=16 * share * step * SUB * LANES,
                transcendentals=0,
            ),
            name="grad",
        )(*given, *extra)

    outer_tiles = tuple(sorted({0, tiles - 1}))
    inner_tiles = tuple(range(1, tiles - 1))
    grad = (grad_part(inner_tiles),) if inner_tiles else ()
    grad = grad_part(outer_tiles, *grad)
    loss = loss + sent(loss, "depth", swap)
    for at in range(1, len(rounds) - 1):
        loss = rays_sum(at, loss)
    squares = [loss]
    if len(rounds) > 1:
        squares += [sent(loss, "rays", pairs) for pairs in rounds[-1]]
    scale = 1.0 / (3.0 * ray_count * groups)
    mean = pl.pallas_call(
        functools.partial(mean_kernel, scale),
        out_shape=jax.ShapeDtypeStruct((1, 1), f32),
        in_specs=[whole] * len(squares),
        out_specs=whole,
        compiler_params=small,
        name="mean",
    )(*squares)
    grad = jnp.swapaxes(grad, 1, 2).reshape(samples, ray_count)
    return grad, mean[0, 0]


def solution(mesh):
    in_specs = (P("depth", "rays"), P(None, "depth", "rays"), P(None, "rays"))
    out_specs = (P("depth", "rays"), P())
    return jax.shard_map(
        on_device, mesh=mesh, in_specs=in_specs, out_specs=out_specs, check_vma=False
    )
```
